32 devices in a mesh: dp: 8 (over z, core), tensor: 4 (over y, x).
Axes of the slice: x: 2, y: 2, z: 4, core: 2. Of those that a mesh axis runs over, the one named last changes fastest.
Arguments:
- tokens: bfloat16 [1024, 2048], P(('dp', 'tensor')), may hold values from -6 to 6
- gate_weight: bfloat16 [2048, 8192], P(None, 'tensor'), may hold values from -0.125 to 0.125
- up_act: bfloat16 [1024, 8192], P('dp', 'tensor'), may hold values from -6 to 6
- cotangent: bfloat16 [1024, 8192], P('dp', 'tensor'), may hold values from -6 to 6
- moment1: bfloat16 [2048, 8192], P('dp', 'tensor'), may hold values from -0.359375 to 0.359375
- moment2: bfloat16 [2048, 8192], P('dp', 'tensor'), may hold values from 0.0039978027 to 0.039794922
Outputs:
- in_grad: bfloat16 [1024, 2048], P(('dp', 'tensor'))
- up_grad: bfloat16 [1024, 8192], P('dp', 'tensor')
- new_moment1: bfloat16 [2048, 8192], P('dp', 'tensor')
- new_moment2: bfloat16 [2048, 8192], P('dp', 'tensor')
- update: float32 [2048, 8192], P('dp', 'tensor')
The draws below stay inside these ranges and needn't reach their ends.
All inputs are finite; a program needn't handle non-finite values.
Results may differ from the reference program's by a relative error of at most 0.015.
Values may be sent and summed in bfloat16 or wider, within the bound.
A program may use at most 64 MiB of HBM per device.

```python
import math
import jax
import jax.numpy as jnp
from jax import lax

DW = 2048
FFW = 8192
GROUP = 128
REPLICAS = 8
TENSOR_WAYS = 4
TOKENS = 1024


def strengthened(array, own_key, source, target, parts, factor):
    def block_of(axis_at):
        return (jnp.arange(array.shape[axis_at]) // (array.shape[axis_at] // parts)).reshape((-1,) + (1,) * (array.ndim - 1 - axis_at))

    one_side = jax.random.permutation(own_key, parts)[block_of(target)]
    second = (block_of(target) + parts // 2) % parts
    return jnp.where((block_of(source) == one_side) | (block_of(source) == second), factor * array, array)


def block_levels(rng, shape, cuts, smallest, high):
    def one(position, blocks):
        heights = jax.random.uniform(jax.random.fold_in(jax.random.fold_in(rng, 6), position), (blocks,), jnp.float32, smallest / len(cuts), high / len(cuts))
        return jnp.repeat(jnp.exp(heights), shape[position] // blocks).reshape((-1,) + (1,) * (len(shape) - position - 1))

    factor_of = one(*cuts[0])
    for cut in cuts[1:]:
        factor_of = factor_of * one(*cut)
    return factor_of


def gaussian(stream_key, dims, deviation, most, shards=(), dtype=jnp.bfloat16):
    drawn = jax.random.normal(stream_key, dims, jnp.float32) * deviation
    if len(shards) > 0:
        drawn = block_levels(stream_key, dims, shards, -0.22, 0.18) * drawn
    return jnp.clip(drawn, min=-most, max=most).astype(dtype)


def gaussian_with(stream_key, shape, deviation, bound, shards, heavy, held_as=jnp.bfloat16):
    values = deviation * jax.random.normal(stream_key, shape, jnp.float32)
    if shards:
        values = values * block_levels(stream_key, shape, shards, -0.22, 0.18)
    return jnp.clip(strengthened(values, jax.random.fold_in(stream_key, 3), *heavy), -bound, bound).astype(held_as)


def setup_inputs(seed: int = 0) -> dict:
    keys = jax.random.split(jax.random.key(seed), 7)
    tokens = gaussian_with(keys[0], (TOKENS, DW), 1.0, 6.0, ((0, 32),), (0, 1, 32, 2.75))
    gate_weight = gaussian(keys[1], (DW, FFW), DW ** -0.5, 0.125, ((1, 4),))
    up_act = gaussian(keys[2], (TOKENS, FFW), 1.0, 6.0, ((0, 8), (1, 4)))
    cotangent = gaussian(keys[3], (TOKENS, FFW), 1.0, 6.0, ((0, 8), (1, 4)))
    moment1 = gaussian(keys[4], (DW, FFW), 0.06, 0.359375, ((0, 8), (1, 4)))
    moment2 = jnp.clip(jnp.exp(math.log(0.039794922) - 2.2979944 * jax.random.uniform(keys[5], (DW, FFW), jnp.float32) ** block_levels(keys[5], (DW, FFW), ((0, 8), (1, 4)), -0.2, 0.2)), 0.0039978027, 0.039794922).astype(jnp.bfloat16)
    return dict(tokens=tokens, gate_weight=gate_weight, up_act=up_act, cotangent=cotangent, moment1=moment1, moment2=moment2)


def reference(tokens, gate_weight, up_act, cotangent, moment1, moment2):
    hidden_cols = FFW // TENSOR_WAYS
    token_sets = tokens.reshape(REPLICAS, GROUP, DW)
    up_sets = up_act.reshape(REPLICAS, GROUP, FFW)
    cot_sets = cotangent.reshape(REPLICAS, GROUP, FFW)
    weight_blocks = gate_weight.astype(jnp.float32).reshape(DW, TENSOR_WAYS, hidden_cols)

    def replica(running, operands):
        feature_rows, up_rows, cot_rows = operands
        gate_pre = jnp.dot(feature_rows, gate_weight, preferred_element_type=jnp.float32)
        sigmoid_gate = jax.nn.sigmoid(gate_pre)
        cot_float = cot_rows.astype(jnp.float32)
        up_result = (cot_float * gate_pre * sigmoid_gate).astype(jnp.bfloat16)
        gate_grad = (cot_float * up_rows.astype(jnp.float32) * sigmoid_gate * (1.0 + gate_pre * (1.0 - sigmoid_gate))).astype(jnp.bfloat16)
        pieces = jnp.einsum('gkc,dkc->kgd', gate_grad.astype(jnp.float32).reshape(GROUP, TENSOR_WAYS, hidden_cols), weight_blocks)
        input_rows = lax.optimization_barrier(jnp.sum(pieces.astype(jnp.bfloat16).astype(jnp.float32), axis=0)).astype(jnp.bfloat16)
        partial_value = jnp.dot(feature_rows.T, gate_grad, preferred_element_type=jnp.float32).astype(jnp.bfloat16)
        return (running + partial_value.astype(jnp.float32), (input_rows, up_result))
    start_sum = jnp.zeros((DW, FFW), jnp.float32)
    grad_total, (input_sets, up_results) = lax.scan(replica, start_sum, (token_sets, up_sets, cot_sets))
    grad = grad_total * (1.0 / math.sqrt(REPLICAS * GROUP))
    first = 0.9 * moment1.astype(jnp.float32) + 0.1 * grad
    second = 0.95 * moment2.astype(jnp.float32) + 0.05 * grad * grad
    update = first / (jnp.sqrt(second) + 1e-08)
    return (input_sets.reshape(TOKENS, DW), up_results.reshape(TOKENS, FFW), first.astype(jnp.bfloat16), second.astype(jnp.bfloat16), update)
```

```python
import functools
import math

import jax
import jax.numpy as jnp
from jax import lax
from jax.experimental import pallas as pl
from jax.experimental.pallas import tpu as pltpu
from jax.sharding import PartitionSpec as P

MESH = pl.DeviceIdType.MESH
F32, BF16 = jnp.float32, jnp.bfloat16
CORES = 2
CHIPS = 4
WIDE = 256
VMEM_BUDGET = 48 * 2**20


def adam(grad, moment1, moment2):
    first = 0.9 * moment1.astype(F32) + 0.1 * grad
    second = 0.95 * moment2.astype(F32) + 0.05 * grad * grad
    return first, second, first / (jnp.sqrt(second) + 1e-08)


def activation_grads(gate_pre, cot, up):
    sig = jax.nn.sigmoid(gate_pre)
    cot = cot.astype(F32)
    up_grad = (cot * gate_pre * sig).astype(BF16)
    gate_grad = (cot * up.astype(F32) * sig * (1.0 + gate_pre * (1.0 - sig))).astype(BF16)
    return up_grad, gate_grad


def flip(t, k):
    bit = 1
    while bit <= k:
        if k & bit:
            t = t + bit - 2 * bit * lax.rem(t // bit, 2)
        bit *= 2
    return t


def kernel(ndp, nt, tok, w, up, cot, m1, m2, in_grad, up_grad, nm1, nm2, upd,
           tg, xg, xt, wv, upv, cotv, m1v, m2v, gall, term, termr,
           loc_sem, w_sem, cu_sem, tg_s, tg_r, x1_s, x1_r, x2_s, x2_r,
           zs, zr, fs, ms, mr, ts, tr):
    d, t = lax.axis_index("dp"), lax.axis_index("tensor")
    z, core = d // CORES, lax.rem(d, CORES)
    mate = d + 1 - 2 * core
    m, dw = tok.shape
    g, hid = up.shape
    rw = m1.shape[0]
    nc, _, hc = wv.shape
    scale = 1.0 / math.sqrt(ndp * g)

    half = z // 2
    near = z + 1 - 2 * lax.rem(z, 2)
    across = 2 - half
    far = 3 - 3 * half
    outer = lax.rem(z + half + 1, 2)
    chips = (near, across, far, z)
    NEAR, ACROSS, FAR, OWN = range(4)

    def rdma(src, dst, s, r, dp, tn):
        return pltpu.make_async_remote_copy(
            src_ref=src, dst_ref=dst, send_sem=s, recv_sem=r, device_id=(dp, tn), device_id_type=MESH)

    def rows_of(i, size):
        return pl.ds(pl.multiple_of(i * size, size), size)

    load_tok = pltpu.make_async_copy(tok, tg.at[0:m], loc_sem.at[0])
    load_x = pltpu.make_async_copy(tok.at[:, rows_of(d, rw)], xg.at[0, d], loc_sem.at[1])
    load_m1 = pltpu.make_async_copy(m1, m1v, loc_sem.at[2])
    load_m2 = pltpu.make_async_copy(m2, m2v, loc_sem.at[3])

    def w_load(c):
        return pltpu.make_async_copy(w.at[:, rows_of(c, hc)], wv.at[c], w_sem.at[c])

    def cu_loads(k):
        src = rows_of(flip(t, k), m)
        dst = pl.ds(k * m, m)
        return (pltpu.make_async_copy(cot.at[src], cotv.at[dst], cu_sem.at[0, k]),
                pltpu.make_async_copy(up.at[src], upv.at[dst], cu_sem.at[1, k]))

    load_tok.start()
    w_load(0).start()
    for copy in cu_loads(0):
        copy.start()
    for c in range(1, nc):
        w_load(c).start()
    load_x.start()

    barrier = pltpu.get_barrier_semaphore()
    for k in range(1, ndp):
        pl.semaphore_signal(barrier, inc=1, device_id=(lax.rem(d + k, ndp), t), device_id_type=MESH)
    for k in range(1, nt):
        pl.semaphore_signal(barrier, inc=1, device_id=(d, flip(t, k)), device_id_type=MESH)
    for k in range(1, nt):
        for copy in cu_loads(k):
            copy.start()
    load_m1.start()
    load_m2.start()

    def tok_copy(k):
        return rdma(tg.at[0:m], tg.at[k * m:(k + 1) * m], tg_s.at[k], tg_r.at[k], d, flip(t, k))

    def x1_copy(k):
        to = lax.rem(d + k, ndp)
        return rdma(tg.at[0:m, rows_of(to, rw)], xg.at[0, d], x1_s.at[k], x1_r.at[k], to, t)

    def x1_recv(k):
        origin = lax.rem(d + ndp - k, ndp)
        return rdma(xg.at[0, origin], xg.at[0, origin], x1_s.at[k], x1_r.at[k], lax.rem(d + k, ndp), t)

    def x2_copy(k):
        return rdma(xg.at[0], xg.at[k], x2_s.at[k], x2_r.at[k], d, flip(t, k))

    def term_copy(k):
        return rdma(term.at[k * m:(k + 1) * m], termr.at[k], ts.at[k], tr.at[k], d, flip(t, k))

    def block(c, part, chip, cr):
        start = pl.multiple_of((chip * CORES + cr) * g, g) + (m if part else 0)
        return gall.at[c, pl.ds(pl.multiple_of(start, m), g - m if part else m)]

    def own_copy(c, part, to):
        b = block(c, part, z, core)
        if to == NEAR:
            return rdma(b, b, zs.at[0, part, c], zr.at[NEAR, part, c], near * CORES + core, t)
        return rdma(b, b, zs.at[1, part, c], zr.at[ACROSS + outer, part, c], across * CORES + core, t)

    def arrival(c, part, origin):
        b = block(c, part, chips[origin], core)
        return rdma(b, b, zs.at[0, part, c], zr.at[origin, part, c], near * CORES + core, t)

    def forward_copy(c, part, origin):
        b = block(c, part, chips[origin], core)
        return rdma(b, b, fs.at[origin - 1, part, c], zr.at[origin, part, c], near * CORES + core, t)

    def mate_copy(c, part, origin):
        b = block(c, part, chips[origin], core)
        return rdma(b, b, ms.at[origin, part, c], mr.at[origin, part, c], mate, t)

    def mate_recv(c, part, origin):
        b = block(c, part, chips[origin], 1 - core)
        return rdma(b, b, ms.at[origin, part, c], mr.at[origin, part, c], mate, t)

    def take(c, part, origin):
        arrival(c, part, origin).wait_recv()
        if origin != NEAR:
            @pl.when(outer == 0)
            def _():
                forward_copy(c, part, origin).start()
        mate_copy(c, part, origin).start()

    def grads(c, part):
        here = slice(m, g) if part else slice(0, m)
        cols = rows_of(c, hc)
        gate_pre = jnp.dot(tg[here], wv[c], preferred_element_type=F32)
        ug, gg = activation_grads(gate_pre, cotv[here, cols], upv[here, cols])
        start = pl.multiple_of(d * g, g) + (m if part else 0)
        gall[c, pl.ds(pl.multiple_of(start, m), g - m if part else m), :] = gg
        for k in range(1, nt) if part else (0,):
            low = (k - 1) * m if part else 0
            up_grad[rows_of(flip(t, k), m), cols] = ug[low:low + m]

    def send_own(c, part):
        own_copy(c, part, ACROSS).start()
        own_copy(c, part, NEAR).start()
        mate_copy(c, part, OWN).start()

    load_tok.wait()
    for copy in cu_loads(0):
        copy.wait()

    @pl.loop(0, nc)
    def _(c):
        w_load(c).wait()
        grads(c, 0)

    load_x.wait()
    pl.semaphore_wait(barrier, ndp - 1 + nt - 1)
    for k in range(1, nt):
        tok_copy(k).start()

    @pl.loop(0, nc)
    def _(c):
        send_own(c, 0)

    for k in range(1, ndp):
        x1_copy(k).start()
    for k in range(1, nt):
        for copy in cu_loads(k):
            copy.wait()

    @pl.when(outer == 0)
    def _():
        @pl.loop(0, nc)
        def _(c):
            take(c, 0, ACROSS)
            take(c, 0, FAR)

    for k in range(1, nt):
        tok_copy(k).wait_recv()

    @pl.loop(0, nc)
    def _(c):
        grads(c, 1)

        @pl.when(c > 0)
        def _():
            send_own(c - 1, 1)

    part = dw // nc

    def term_part(n):
        rows = rows_of(n, part)
        own = rows_of(d, g)
        total = jnp.zeros((g, part), F32)
        for c in range(nc):
            total += lax.dot_general(
                gall[c, own, :], wv[c, rows, :], (((1,), (1,)), ((), ())), preferred_element_type=F32)
        term[:, rows] = total.astype(BF16)

    term_part(0)
    send_own(nc - 1, 1)
    for k in range(1, ndp):
        x1_recv(k).wait_recv()
    for k in range(1, nt):
        x2_copy(k).start()

    @pl.loop(1, nc)
    def _(n):
        term_part(n)

    @pl.when(outer == 1)
    def _():
        @pl.loop(0, nc)
        def _(c):
            take(c, 0, ACROSS)
            take(c, 0, FAR)

    for k in range(1, nt):
        term_copy(k).start()

    @pl.loop(0, nc)
    def _(c):
        take(c, 0, NEAR)

    for k in range(1, nt):
        x2_copy(k).wait_recv()
    for i in range(ndp):
        xt[:, i * g:(i + 1) * g] = xg[:, i].reshape(g, rw).T

    total = term[0:m, :].astype(F32)
    for k in range(1, nt):
        term_copy(k).wait_recv()
        total += termr[k].astype(F32)
    in_grad[...] = total.astype(BF16)
    load_m1.wait()
    load_m2.wait()

    def update(c):
        for origin in range(4):
            for part in range(2):
                mate_recv(c, part, origin).wait_recv()
        cols = rows_of(c, hc)
        grad = jnp.dot(xt[...], gall[c], preferred_element_type=F32) * scale
        first, second, step = adam(grad, m1v[:, cols], m2v[:, cols])
        nm1[:, cols] = first.astype(BF16)
        nm2[:, cols] = second.astype(BF16)
        upd[:, cols] = step

    @pl.loop(0, nc + 1)
    def _(c):
        @pl.when(c < nc)
        def _():
            take(c, 1, NEAR)
            take(c, 1, ACROSS)
            take(c, 1, FAR)

        @pl.when(c > 0)
        def _():
            update(c - 1)

    for k in range(1, nt):
        tok_copy(k).wait_send()
        x2_copy(k).wait_send()
        term_copy(k).wait_send()
    for k in range(1, ndp):
        x1_copy(k).wait_send()

    @pl.loop(0, nc)
    def _(c):
        for p in range(2):
            own_copy(c, p, NEAR).wait_send()
            own_copy(c, p, ACROSS).wait_send()
            for origin in range(4):
                mate_copy(c, p, origin).wait_send()

            @pl.when(outer == 0)
            def _():
                forward_copy(c, p, ACROSS).wait_send()
                forward_copy(c, p, FAR).wait_send()


def fused(ndp, nt, tokens, gate_weight, up_act, cotangent, moment1, moment2):
    m, dw = tokens.shape
    g, hid = up_act.shape
    rw = moment1.shape[0]
    nc = hid // WIDE
    any_spec, vmem = pl.BlockSpec(memory_space=pltpu.HBM), pl.BlockSpec(memory_space=pltpu.VMEM)
    dma = pltpu.SemaphoreType.DMA
    results = (((m, dw), BF16), ((g, hid), BF16), ((rw, hid), BF16), ((rw, hid), BF16), ((rw, hid), F32))
    held = pl.pallas_call(
        functools.partial(kernel, ndp, nt),
        out_shape=tuple(pltpu.VMEM(shape, dtype) for shape, dtype in results),
        in_specs=[any_spec] * 6,
        out_specs=(vmem,) * 5,
        scratch_shapes=[
            pltpu.VMEM((g, dw), BF16),
            pltpu.VMEM((nt, ndp, m, rw), BF16),
            pltpu.VMEM((rw, ndp * g), BF16),
            pltpu.VMEM((nc, dw, WIDE), BF16),
            pltpu.VMEM((g, hid), BF16),
            pltpu.VMEM((g, hid), BF16),
            pltpu.VMEM((rw, hid), BF16),
            pltpu.VMEM((rw, hid), BF16),
            pltpu.VMEM((nc, ndp * g, WIDE), BF16),
            pltpu.VMEM((g, dw), BF16),
            pltpu.VMEM((nt, m, dw), BF16),
            dma((4,)), dma((nc,)), dma((2, nt)),
            dma((nt,)), dma((nt,)),
            dma((ndp,)), dma((ndp,)),
            dma((nt,)), dma((nt,)),
            dma((2, 2, nc)), dma((3, 2, nc)), dma((2, 2, nc)),
            dma((4, 2, nc)), dma((4, 2, nc)),
            dma((nt,)), dma((nt,)),
        ],
        compiler_params=pltpu.CompilerParams(
            collective_id=0, has_side_effects=True, vmem_limit_bytes=VMEM_BUDGET),
    )(*(pltpu.with_memory_space_constraint(x, pltpu.HBM)
        for x in (tokens, gate_weight, up_act, cotangent, moment1, moment2)))
    return pl.pallas_call(
        write_out,
        out_shape=tuple(pltpu.HBM(shape, dtype) for shape, dtype in results),
        in_specs=[vmem] * 5,
        out_specs=(any_spec,) * 5,
        scratch_shapes=[dma((5,))],
        compiler_params=pltpu.CompilerParams(vmem_limit_bytes=2**20),
    )(*(pltpu.with_memory_space_constraint(x, pltpu.VMEM) for x in held))


def write_out(*refs):
    sems = refs[-1]
    copies = [pltpu.make_async_copy(refs[i], refs[5 + i], sems.at[i]) for i in range(5)]
    for copy in reversed(copies):
        copy.start()
    for copy in copies:
        copy.wait()


def plain(ndp, nt, tokens, gate_weight, up_act, cotangent, moment1, moment2):
    gathered = lax.all_gather(tokens, "tensor", axis=0, tiled=True)
    gate_pre = jnp.dot(gathered, gate_weight, preferred_element_type=F32)
    up_grad, gate_grad = activation_grads(gate_pre, cotangent, up_act)
    term = lax.dot_general(
        gate_grad, gate_weight, (((1,), (1,)), ((), ())), preferred_element_type=F32).astype(BF16)
    in_grad = lax.psum_scatter(term, "tensor", scatter_dimension=0, tiled=True)
    partial_value = lax.dot_general(
        gathered, gate_grad, (((0,), (0,)), ((), ())), preferred_element_type=F32).astype(BF16)
    shard = lax.psum_scatter(partial_value.astype(F32), "dp", scatter_dimension=0, tiled=True)
    first, second, update = adam(shard * (1.0 / math.sqrt(ndp * gathered.shape[0])), moment1, moment2)
    return in_grad, up_grad, first.astype(BF16), second.astype(BF16), update


def local(ndp, nt, *args):
    (m, dw), (g, hid), rw = args[0].shape, args[2].shape, args[4].shape[0]
    need = (2 * dw * hid + 2 * ndp * g * (hid + 2 * rw) + 12 * g * hid + 16 * rw * hid + 16 * g * dw)
    fits = (need <= VMEM_BUDGET and ndp == CORES * CHIPS and nt > 1 and nt & (nt - 1) == 0
            and hid % WIDE == 0 and g % 128 == 0 and rw % 128 == 0 and m % 16 == 0
            and dw % (128 * (hid // WIDE)) == 0)
    return (fused if fits else plain)(ndp, nt, *args)


def solution(mesh):
    both = P("dp", "tensor")
    rows = P(("dp", "tensor"), None)
    return jax.shard_map(
        functools.partial(local, mesh.shape["dp"], mesh.shape["tensor"]),
        mesh=mesh,
        in_specs=(rows, P(None, "tensor"), both, both, both, both),
        out_specs=(rows, both, both, both, both),
        check_vma=False,
    )
```

```python
import functools
import math

import jax
import jax.numpy as jnp
from jax import lax
from jax.experimental import pallas as pl
from jax.experimental.pallas import tpu as pltpu
from jax.sharding import PartitionSpec as P

MESH = pl.DeviceIdType.MESH
F32, BF16 = jnp.float32, jnp.bfloat16
CORES = 2
CHIPS = 4
WIDE = 256
SUMMED = 4
LEAD = 4
W_DEPTH = 3
VMEM_BUDGET = 48 * 2**20


def adam(grad, moment1, moment2):
    first = 0.9 * moment1.astype(F32) + 0.1 * grad
    second = 0.95 * moment2.astype(F32) + 0.05 * grad * grad
    return first, second, first / (jnp.sqrt(second) + 1e-08)


def activation_grads(gate_pre, cot, up):
    sig = jax.nn.sigmoid(gate_pre)
    cot = cot.astype(F32)
    up_grad = (cot * gate_pre * sig).astype(BF16)
    gate_grad = (cot * up.astype(F32) * sig * (1.0 + gate_pre * (1.0 - sig))).astype(BF16)
    return up_grad, gate_grad


def phase(run):
    with jax.named_scope(run.__name__):
        run()


def flip(t, k):
    bit = 1
    while bit <= k:
        if k & bit:
            t = t + bit - 2 * bit * lax.rem(t // bit, 2)
        bit *= 2
    return t


def kernel(ndp, nt, tok, w, up, cot, m1, m2, in_grad, up_grad, nm1, nm2, upd,
           tg, xg, xp, xt, xtp, wv, upv, cotv, m1v, m2v, gall, term, termr, part_s, part_r,
           loc_sem, w_sem, cu_sem, tg_s, tg_r, x_s, x_r, xp_r, xf_sem, x2_s, x2_r, xp2_s, xp2_r,
           zs, zr, fs, ms, mr, rs, rr, ts, tr):
    d, t = lax.axis_index("dp"), lax.axis_index("tensor")
    z, core = d // CORES, lax.rem(d, CORES)
    mate = d + 1 - 2 * core
    m, dw = tok.shape
    g, hid = up.shape
    rw = m1.shape[0]
    nc, _, hc = wv.shape
    nr = part_s.shape[0]
    ng = nc - nr
    lead = min(LEAD, ng)
    scale = 1.0 / math.sqrt(ndp * g)

    half = z // 2
    near = z + 1 - 2 * lax.rem(z, 2)
    across = 2 - half
    far = 3 - 3 * half
    outer = lax.rem(z + half + 1, 2)
    chips = (near, across, far, z)
    NEAR, ACROSS, FAR, OWN = range(4)
    seen = ACROSS + outer
    first_rep = CORES * (1 - half)
    others = ndp - CORES
    beyond = others - CORES

    def inner_only(run):
        pl.when(outer == 0)(run)

    def outer_only(run):
        pl.when(outer == 1)(run)

    def rdma(src, dst, s, r, dp, tn):
        return pltpu.make_async_remote_copy(
            src_ref=src, dst_ref=dst, send_sem=s, recv_sem=r, device_id=(dp, tn), device_id_type=MESH)

    def rows_of(i, size):
        return pl.ds(pl.multiple_of(i * size, size), size)

    load_tok = pltpu.make_async_copy(tok, tg.at[0:m], loc_sem.at[0])
    load_x = pltpu.make_async_copy(tok.at[:, rows_of(d, rw)], xg.at[0, d], loc_sem.at[1])
    load_xp = pltpu.make_async_copy(
        tok.at[:, rows_of(near * CORES + core, rw)], xp.at[0, d - first_rep], loc_sem.at[4])
    load_m1 = pltpu.make_async_copy(m1, m1v, loc_sem.at[2])
    load_m2 = pltpu.make_async_copy(m2, m2v, loc_sem.at[3])

    def w_load(c):
        return pltpu.make_async_copy(w.at[:, rows_of(c, hc)], wv.at[c], w_sem.at[c])

    def cu_loads(k):
        src = rows_of(flip(t, k), m)
        dst = pl.ds(k * m, m)
        return (pltpu.make_async_copy(cot.at[src], cotv.at[dst], cu_sem.at[0, k]),
                pltpu.make_async_copy(up.at[src], upv.at[dst], cu_sem.at[1, k]))

    def tok_copy(k):
        return rdma(tg.at[0:m], tg.at[k * m:(k + 1) * m], tg_s.at[k], tg_r.at[k], d, flip(t, k))

    def features(chip, cr):
        return tg.at[0:m, rows_of(chip * CORES + cr, rw)]

    def x_near(cr):
        return rdma(features(near, cr), xg.at[0, d], x_s.at[cr], x_r.at[NEAR, core], near * CORES + cr, t)

    def x_across(cr):
        return rdma(features(across, cr), xg.at[0, d], x_s.at[2 + cr], x_r.at[seen, core],
                    across * CORES + cr, t)

    def xp_across(cr):
        return rdma(features(far, cr), xp.at[0, d - CORES * half], x_s.at[4 + cr], xp_r.at[seen, core],
                    across * CORES + cr, t)

    def x_mate():
        return rdma(features(z, 1 - core), xg.at[0, d], x_s.at[6], x_r.at[OWN, core], mate, t)

    def xp_mate():
        return rdma(features(near, 1 - core), xp.at[0, d - first_rep], x_s.at[7], xp_r.at[OWN, core], mate, t)

    def x_forward():
        return rdma(xp.at[0, pl.ds(first_rep, beyond)], xg.at[0, pl.ds(2 * first_rep, beyond)],
                    xf_sem.at[0], xf_sem.at[1], near * CORES + core, t)

    def xf_recv():
        return rdma(xp.at[0, 0:beyond], xg.at[0, pl.ds(CORES * CORES * (1 - half), beyond)],
                    xf_sem.at[0], xf_sem.at[1], near * CORES + core, t)

    def x_recv(origin, cr):
        return rdma(xg.at[0, d], xg.at[0, chips[origin] * CORES + cr], x_s.at[0], x_r.at[origin, cr], mate, t)

    def xp_recv(origin, cr):
        return rdma(xg.at[0, d], xp.at[0, chips[origin] * CORES + cr - first_rep], x_s.at[0],
                    xp_r.at[origin, cr], mate, t)

    def x2_copy(k):
        return rdma(xg.at[0], xg.at[k], x2_s.at[k], x2_r.at[k], d, flip(t, k))

    def xp2_copy(k):
        return rdma(xp.at[0], xp.at[k], xp2_s.at[k], xp2_r.at[k], d, flip(t, k))

    def term_copy(k):
        return rdma(term.at[k * m:(k + 1) * m], termr.at[k], ts.at[k], tr.at[k], d, flip(t, k))

    def block(c, part, chip, cr):
        start = pl.multiple_of((chip * CORES + cr) * g, g) + (m if part else 0)
        return gall.at[c, pl.ds(pl.multiple_of(start, m), g - m if part else m)]

    def own_copy(c, part, to):
        b = block(c, part, z, core)
        if to == NEAR:
            return rdma(b, b, zs.at[0, part, c], zr.at[NEAR, part, c], near * CORES + core, t)
        return rdma(b, b, zs.at[1, part, c], zr.at[seen, part, c], across * CORES + core, t)

    def arrival(c, part, origin):
        b = block(c, part, chips[origin], core)
        return rdma(b, b, zs.at[0, part, c], zr.at[origin, part, c], near * CORES + core, t)

    def forward_copy(c, part, origin):
        b = block(c, part, chips[origin], core)
        return rdma(b, b, fs.at[origin - 1, part, c], zr.at[origin, part, c], near * CORES + core, t)

    def mate_copy(c, part, origin):
        b = block(c, part, chips[origin], core)
        return rdma(b, b, ms.at[origin, part, c], mr.at[origin, part, c], mate, t)

    def mate_recv(c, part, origin):
        b = block(c, part, chips[origin], 1 - core)
        return rdma(b, b, ms.at[origin, part, c], mr.at[origin, part, c], mate, t)

    def part_copy(j):
        return rdma(part_s.at[j], part_r.at[j], rs.at[j], rr.at[j], near * CORES + core, t)

    def take(c, part, origin, pass_on=True):
        arrival(c, part, origin).wait_recv()
        if origin != NEAR and pass_on:
            @inner_only
            def _():
                forward_copy(c, part, origin).start()
        mate_copy(c, part, origin).start()

    def grads(c, part):
        here = slice(m, g) if part else slice(0, m)
        cols = rows_of(c, hc)
        gate_pre = jnp.dot(tg[here], wv[c], preferred_element_type=F32)
        ug, gg = activation_grads(gate_pre, cotv[here, cols], upv[here, cols])
        start = pl.multiple_of(d * g, g) + (m if part else 0)
        gall[c, pl.ds(pl.multiple_of(start, m), g - m if part else m), :] = gg
        for k in range(1, nt) if part else (0,):
            low = (k - 1) * m if part else 0
            up_grad[rows_of(flip(t, k), m), cols] = ug[low:low + m]

    def near_copies(c, run):
        pl.when(jnp.logical_or(outer == 1, c < ng))(run)

    def send_own(c, part):
        own_copy(c, part, ACROSS).start()

        def to_near():
            own_copy(c, part, NEAR).start()
        near_copies(c, to_near)
        mate_copy(c, part, OWN).start()

    span = dw // nc

    def term_part(n):
        rows = rows_of(n, span)
        own = rows_of(d, g)
        total = jnp.zeros((g, span), F32)
        for c in range(nc):
            total += lax.dot_general(
                gall[c, own, :], wv[c, rows, :], (((1,), (1,)), ((), ())), preferred_element_type=F32)
        term[:, rows] = total.astype(BF16)

    def mates_wait(c, origins):
        for origin in origins:
            for part in range(2):
                mate_recv(c, part, origin).wait_recv()

    def step(c, grad):
        cols = rows_of(c, hc)
        first, second, change = adam(grad * scale, m1v[:, cols], m2v[:, cols])
        nm1[:, cols] = first.astype(BF16)
        nm2[:, cols] = second.astype(BF16)
        upd[:, cols] = change

    def update(c, origins=(OWN, NEAR, ACROSS, FAR)):
        mates_wait(c, origins)
        step(c, jnp.dot(xt[...], gall[c], preferred_element_type=F32))

    def reduce(c, j):
        mates_wait(c, (OWN, ACROSS, FAR))
        rows = pl.ds(pl.multiple_of(first_rep * g, g), others * g)
        part_s[j] = jnp.dot(xtp[...], gall[c, rows, :], preferred_element_type=F32).astype(BF16)
        part_copy(j).start()

    def finish(c, j):
        mates_wait(c, (OWN,))
        own = rows_of(z, CORES * g)
        grad = jnp.dot(xt[:, own], gall[c, own, :], preferred_element_type=F32)
        part_copy(j).wait_recv()
        step(c, grad + part_r[j].astype(F32))

    depth = min(W_DEPTH, nc)

    load_tok.start()
    for copy in cu_loads(0):
        copy.start()
    for c in range(depth):
        w_load(c).start()

    barrier = pltpu.get_barrier_semaphore()

    def greet(dp, tn):
        pl.semaphore_signal(barrier, inc=1, device_id=(dp, tn), device_id_type=MESH)

    for k in range(1, nt):
        greet(d, flip(t, k))
    greet(mate, t)
    for cr in range(CORES):
        greet(near * CORES + cr, t)

    @inner_only
    def _():
        for chip in (across, far):
            for cr in range(CORES):
                greet(chip * CORES + cr, t)

    @phase
    def tok_load():
        load_tok.wait()

    @phase
    def meet():
        pl.semaphore_wait(barrier, nt - 1 + 1 + 2 * CORES)

    for k in range(1, nt):
        tok_copy(k).start()

    @phase
    def own_loads():
        for copy in cu_loads(0):
            copy.wait()

    @phase
    def own_grads():
        @pl.loop(0, nc)
        def _(c):
            w_load(c).wait()

            @pl.when(c + depth < nc)
            def _():
                w_load(c + depth).start()
            grads(c, 0)

            @pl.when(c > 0)
            def _():
                send_own(c - 1, 0)

    for k in range(1, nt):
        for copy in cu_loads(k):
            copy.start()
    load_x.start()
    inner_only(load_xp.start)
    load_m1.start()
    load_m2.start()
    send_own(nc - 1, 0)
    for cr in range(CORES):
        xp_across(cr).start()
    for cr in range(CORES):
        x_across(cr).start()
        x_near(cr).start()
    x_mate().start()
    inner_only(lambda: xp_mate().start())

    @phase
    def inner_forwards():
        @inner_only
        def _():
            @pl.loop(0, ng)
            def _(c):
                take(c, 0, ACROSS)
                take(c, 0, FAR)

    @phase
    def tok_wait():
        for k in range(1, nt):
            for copy in cu_loads(k):
                copy.wait()
        for k in range(1, nt):
            tok_copy(k).wait_recv()

    @phase
    def other_grads():
        @pl.loop(0, nc)
        def _(c):
            grads(c, 1)

            @pl.when(c > 0)
            def _():
                send_own(c - 1, 1)

    @phase
    def x_exchange():
        term_part(0)
        send_own(nc - 1, 1)
        load_x.wait()
        x_recv(OWN, 1 - core).wait_recv()
        for cr in range(CORES):
            x_recv(NEAR, cr).wait_recv()

        @inner_only
        def _():
            for origin in (ACROSS, FAR):
                for cr in range(CORES):
                    xp_recv(origin, cr).wait_recv()
            x_forward().start()
            load_xp.wait()
            xp_recv(OWN, 1 - core).wait_recv()
            for origin in (ACROSS, FAR):
                for cr in range(CORES):
                    x_recv(origin, cr).wait_recv()
            for k in range(1, nt):
                x2_copy(k).start()
            for k in range(1, nt):
                xp2_copy(k).start()

    @phase
    def terms():
        @pl.loop(1, nc)
        def _(n):
            term_part(n)

    @phase
    def outer_takes():
        @outer_only
        def _():
            xf_recv().wait_recv()
            for k in range(1, nt):
                x2_copy(k).start()

            @pl.loop(0, ng)
            def _(c):
                take(c, 0, ACROSS)
                take(c, 0, FAR)

    for k in range(1, nt):
        term_copy(k).start()

    @phase
    def near_takes():
        @pl.loop(0, ng)
        def _(c):
            take(c, 0, NEAR)

        @inner_only
        def _():
            @pl.loop(ng, nc)
            def _(c):
                for origin in (NEAR, ACROSS, FAR):
                    take(c, 0, origin, False)

    def takes(c):
        @phase
        def others_in():
            for origin in (NEAR, ACROSS, FAR):
                take(c, 1, origin)

    @pl.loop(0, lead)
    def _(c):
        takes(c)

    @phase
    def x_wait():
        for k in range(1, nt):
            x2_copy(k).wait_recv()

    load_m1.wait()
    load_m2.wait()

    @phase
    def transposes():
        for i in range(ndp):
            xt[:, i * g:(i + 1) * g] = xg[:, i].reshape(g, rw).T

    @pl.loop(lead, ng)
    def _(c):
        takes(c)

        @phase
        def updates():
            update(c - lead)

    def input_grads():
        with jax.named_scope("input_grads"):
            total = term[0:m, :].astype(F32)
            for k in range(1, nt):
                term_copy(k).wait_recv()
                total += termr[k].astype(F32)
            in_grad[...] = total.astype(BF16)

    @inner_only
    def _():
        @phase
        def xp_wait():
            for k in range(1, nt):
                xp2_copy(k).wait_recv()
            for i in range(others):
                xtp[:, i * g:(i + 1) * g] = xp[:, i].reshape(g, rw).T

        for j in range(nr):
            @phase
            def last_in():
                for origin in (ACROSS, FAR, NEAR):
                    take(ng + j, 1, origin, False)

            @phase
            def updates():
                update(ng - lead + j)

            @phase
            def reduces():
                reduce(ng + j, j)

        @pl.loop(ng - lead + nr, ng)
        def _(c):
            update(c)

        @pl.loop(ng, nc)
        def _(c):
            update(c, (NEAR,))
        input_grads()

    @outer_only
    def _():
        @pl.loop(ng - lead, ng)
        def _(c):
            @phase
            def updates():
                update(c)
        input_grads()
        for j in range(nr):
            @phase
            def finishes():
                finish(ng + j, j)

    @phase
    def drain():
        for k in range(1, nt):
            tok_copy(k).wait_send()
            x2_copy(k).wait_send()
            term_copy(k).wait_send()
        for cr in range(CORES):
            x_near(cr).wait_send()
            x_across(cr).wait_send()
            xp_across(cr).wait_send()
        x_mate().wait_send()

        @pl.loop(0, nc)
        def _(c):
            for p in range(2):
                own_copy(c, p, ACROSS).wait_send()
                near_copies(c, own_copy(c, p, NEAR).wait_send)
                mate_copy(c, p, OWN).wait_send()

        @pl.loop(0, ng)
        def _(c):
            for p in range(2):
                for origin in (NEAR, ACROSS, FAR):
                    mate_copy(c, p, origin).wait_send()

        @inner_only
        def _():
            xp_mate().wait_send()
            x_forward().wait_send()
            for k in range(1, nt):
                xp2_copy(k).wait_send()

            @pl.loop(0, ng)
            def _(c):
                for p in range(2):
                    forward_copy(c, p, ACROSS).wait_send()
                    forward_copy(c, p, FAR).wait_send()

            @pl.loop(ng, nc)
            def _(c):
                for p in range(2):
                    for origin in (NEAR, ACROSS, FAR):
                        mate_copy(c, p, origin).wait_send()
            for j in range(nr):
                part_copy(j).wait_send()


def fused(ndp, nt, tokens, gate_weight, up_act, cotangent, moment1, moment2):
    m, dw = tokens.shape
    g, hid = up_act.shape
    rw = moment1.shape[0]
    nc = hid // WIDE
    nr = nc // SUMMED
    any_spec, vmem = pl.BlockSpec(memory_space=pltpu.HBM), pl.BlockSpec(memory_space=pltpu.VMEM)
    dma = pltpu.SemaphoreType.DMA
    results = (((m, dw), BF16), ((g, hid), BF16), ((rw, hid), BF16), ((rw, hid), BF16), ((rw, hid), F32))
    held = pl.pallas_call(
        functools.partial(kernel, ndp, nt),
        out_shape=tuple(pltpu.VMEM(shape, dtype) for shape, dtype in results),
        in_specs=[any_spec] * 6,
        out_specs=(vmem,) * 5,
        scratch_shapes=[
            pltpu.VMEM((g, dw), BF16),
            pltpu.VMEM((nt, ndp, m, rw), BF16),
            pltpu.VMEM((nt, ndp - CORES, m, rw), BF16),
            pltpu.VMEM((rw, ndp * g), BF16),
            pltpu.VMEM((rw, (ndp - CORES) * g), BF16),
            pltpu.VMEM((nc, dw, WIDE), BF16),
            pltpu.VMEM((g, hid), BF16),
            pltpu.VMEM((g, hid), BF16),
            pltpu.VMEM((rw, hid), BF16),
            pltpu.VMEM((rw, hid), BF16),
            pltpu.VMEM((nc, ndp * g, WIDE), BF16),
            pltpu.VMEM((g, dw), BF16),
            pltpu.VMEM((nt, m, dw), BF16),
            pltpu.VMEM((nr, rw, WIDE), BF16),
            pltpu.VMEM((nr, rw, WIDE), BF16),
            dma((5,)), dma((nc,)), dma((2, nt)),
            dma((nt,)), dma((nt,)),
            dma((8,)), dma((4, CORES)), dma((4, CORES)), dma((2,)),
            dma((nt,)), dma((nt,)), dma((nt,)), dma((nt,)),
            dma((2, 2, nc)), dma((3, 2, nc)), dma((2, 2, nc)),
            dma((4, 2, nc)), dma((4, 2, nc)),
            dma((nr,)), dma((nr,)),
            dma((nt,)), dma((nt,)),
        ],
        compiler_params=pltpu.CompilerParams(
            collective_id=0, has_side_effects=True, vmem_limit_bytes=VMEM_BUDGET),
    )(*(pltpu.with_memory_space_constraint(x, pltpu.HBM)
        for x in (tokens, gate_weight, up_act, cotangent, moment1, moment2)))
    return pl.pallas_call(
        write_out,
        out_shape=tuple(pltpu.HBM(shape, dtype) for shape, dtype in results),
        in_specs=[vmem] * 5,
        out_specs=(any_spec,) * 5,
        scratch_shapes=[dma((5,))],
        compiler_params=pltpu.CompilerParams(vmem_limit_bytes=2**20),
    )(*(pltpu.with_memory_space_constraint(x, pltpu.VMEM) for x in held))


def write_out(*refs):
    sems = refs[-1]
    copies = [pltpu.make_async_copy(refs[i], refs[5 + i], sems.at[i]) for i in range(5)]
    for copy in reversed(copies):
        copy.start()
    for copy in copies:
        copy.wait()


def plain(ndp, nt, tokens, gate_weight, up_act, cotangent, moment1, moment2):
    gathered = lax.all_gather(tokens, "tensor", axis=0, tiled=True)
    gate_pre = jnp.dot(gathered, gate_weight, preferred_element_type=F32)
    up_grad, gate_grad = activation_grads(gate_pre, cotangent, up_act)
    term = lax.dot_general(
        gate_grad, gate_weight, (((1,), (1,)), ((), ())), preferred_element_type=F32).astype(BF16)
    in_grad = lax.psum_scatter(term, "tensor", scatter_dimension=0, tiled=True)
    partial_value = lax.dot_general(
        gathered, gate_grad, (((0,), (0,)), ((), ())), preferred_element_type=F32).astype(BF16)
    shard = lax.psum_scatter(partial_value.astype(F32), "dp", scatter_dimension=0, tiled=True)
    first, second, update = adam(shard * (1.0 / math.sqrt(ndp * gathered.shape[0])), moment1, moment2)
    return in_grad, up_grad, first.astype(BF16), second.astype(BF16), update


def local(ndp, nt, *args):
    (m, dw), (g, hid), rw = args[0].shape, args[2].shape, args[4].shape[0]
    need = (2 * dw * hid + 2 * ndp * g * (hid + 2 * rw) + 12 * g * hid + 16 * rw * hid + 16 * g * dw)
    fits = (need <= VMEM_BUDGET and hid >= 8 * WIDE and ndp == CORES * CHIPS and nt > 1 and nt & (nt - 1) == 0
            and hid % WIDE == 0 and g % 128 == 0 and rw % 128 == 0 and m % 16 == 0
            and dw % (128 * (hid // WIDE)) == 0)
    return (fused if fits else plain)(ndp, nt, *args)


def solution(mesh):
    both = P("dp", "tensor")
    rows = P(("dp", "tensor"), None)
    return jax.shard_map(
        functools.partial(local, mesh.shape["dp"], mesh.shape["tensor"]),
        mesh=mesh,
        in_specs=(rows, P(None, "tensor"), both, both, both, both),
        out_specs=(rows, both, both, both, both),
        check_vma=False,
    )
```

```python
import functools
import math

import jax
import jax.numpy as jnp
from jax import lax
from jax.experimental import pallas as pl
from jax.experimental.pallas import tpu as pltpu
from jax.sharding import PartitionSpec as P

MESH = pl.DeviceIdType.MESH
F32, BF16 = jnp.float32, jnp.bfloat16
CORES = 2
CHIPS = 4
WIDE = 256
SUMMED = 2
LEAD = 4
W_DEPTH = 3
VMEM_BUDGET = 48 * 2**20


def adam(grad, moment1, moment2):
    first = 0.9 * moment1.astype(F32) + 0.1 * grad
    second = 0.95 * moment2.astype(F32) + 0.05 * grad * grad
    return first, second, first / (jnp.sqrt(second) + 1e-08)


def activation_grads(gate_pre, cot, up):
    sig = jax.nn.sigmoid(gate_pre)
    cot = cot.astype(F32)
    up_grad = (cot * gate_pre * sig).astype(BF16)
    gate_grad = (cot * up.astype(F32) * sig * (1.0 + gate_pre * (1.0 - sig))).astype(BF16)
    return up_grad, gate_grad


def phase(run):
    with jax.named_scope(run.__name__):
        run()


def flip(t, k):
    bit = 1
    while bit <= k:
        if k & bit:
            t = t + bit - 2 * bit * lax.rem(t // bit, 2)
        bit *= 2
    return t


def kernel(ndp, nt, tok, w, up, cot, m1, m2, in_grad, up_grad, nm1, nm2, upd,
           tg, xg, xp, xt, xtp, wv, upv, cotv, m1v, m2v, gall, term, termr, part_s, part_r,
           loc_sem, w_sem, cu_sem, tok_sem, x_sem, x2_sem, zs, fs, ms, zr_near, zr_rest,
           mr_near, mr_rest, rs, rr, term_sem):
    d, t = lax.axis_index("dp"), lax.axis_index("tensor")
    z, core = d // CORES, lax.rem(d, CORES)
    mate = d + 1 - 2 * core
    m, dw = tok.shape
    g, hid = up.shape
    rw = m1.shape[0]
    nc, _, hc = wv.shape
    nr = part_s.shape[0]
    ng = nc - nr
    lead = min(LEAD, ng)
    scale = 1.0 / math.sqrt(ndp * g)

    half = z // 2
    near = z + 1 - 2 * lax.rem(z, 2)
    across = 2 - half
    far = 3 - 3 * half
    outer = lax.rem(z + half + 1, 2)
    first_rep = CORES * (1 - half)
    others = ndp - CORES
    beyond = others - CORES

    def inner_only(run):
        pl.when(outer == 0)(run)

    def outer_only(run):
        pl.when(outer == 1)(run)

    def rdma(src, dst, s, r, dp, tn):
        return pltpu.make_async_remote_copy(
            src_ref=src, dst_ref=dst, send_sem=s, recv_sem=r, device_id=(dp, tn), device_id_type=MESH)

    def rows_of(i, size):
        return pl.ds(pl.multiple_of(i * size, size), size)

    served = near * CORES + 1 - core

    load_tok = pltpu.make_async_copy(tok, tg.at[0:m], loc_sem.at[0])
    load_x = pltpu.make_async_copy(tok.at[:, rows_of(d, rw)], xg.at[0, d], loc_sem.at[1])
    load_xp = pltpu.make_async_copy(tok.at[:, rows_of(served, rw)], xp.at[0, d - first_rep], loc_sem.at[4])
    load_m1 = pltpu.make_async_copy(m1, m1v, loc_sem.at[2])
    load_m2 = pltpu.make_async_copy(m2, m2v, loc_sem.at[3])

    def w_load(c):
        return pltpu.make_async_copy(w.at[:, rows_of(c, hc)], wv.at[c], w_sem.at[c])

    def cu_loads(k):
        src = rows_of(flip(t, k), m)
        dst = pl.ds(k * m, m)
        return (pltpu.make_async_copy(cot.at[src], cotv.at[dst], cu_sem.at[1 if k else 0]),
                pltpu.make_async_copy(up.at[src], upv.at[dst], cu_sem.at[2 if k else 0]))

    def cu_wait(first):
        if first:
            pltpu.make_async_copy(cot.at[0:2 * m], cotv.at[0:2 * m], cu_sem.at[0]).wait()
        else:
            pltpu.make_async_copy(cot.at[m:g], cotv.at[m:g], cu_sem.at[1]).wait()
            pltpu.make_async_copy(up.at[m:g], upv.at[m:g], cu_sem.at[2]).wait()

    def tok_copy(k):
        return rdma(tg.at[0:m], tg.at[k * m:(k + 1) * m], tok_sem.at[0], tok_sem.at[1], d, flip(t, k))

    tok_all = rdma(tg.at[m:g], tg.at[m:g], tok_sem.at[0], tok_sem.at[1], mate, t)

    def features(chip, cr):
        return tg.at[0:m, rows_of(chip * CORES + cr, rw)]

    def x_near(cr):
        return rdma(features(near, cr), xg.at[0, d], x_sem.at[0], x_sem.at[1], near * CORES + cr, t)

    def x_across(cr):
        return rdma(features(across, cr), xg.at[0, d], x_sem.at[0], x_sem.at[1], across * CORES + cr, t)

    def xp_across(cr):
        return rdma(features(far, 1 - cr), xp.at[0, d - CORES * half], x_sem.at[0], x_sem.at[2],
                    across * CORES + cr, t)

    x_mate = rdma(features(z, 1 - core), xg.at[0, d], x_sem.at[0], x_sem.at[1], mate, t)
    xp_mate = rdma(features(near, core), xp.at[0, d - first_rep], x_sem.at[3], x_sem.at[4], mate, t)
    x_forward = rdma(xp.at[0, pl.ds(first_rep, beyond)], xg.at[0, pl.ds(CORES * first_rep, beyond)],
                     x_sem.at[5], x_sem.at[1], served, t)
    x_all = rdma(xg.at[0, 0:ndp - 1], xg.at[0, 0:ndp - 1], x_sem.at[0], x_sem.at[1], mate, t)
    xp_beyond = rdma(xp.at[0, 0:beyond], xp.at[0, 0:beyond], x_sem.at[5], x_sem.at[2], mate, t)

    def x2_copy(k):
        return rdma(xg.at[0], xg.at[k], x2_sem.at[0], x2_sem.at[1], d, flip(t, k))

    def xp2_copy(k):
        return rdma(xp.at[0], xp.at[k], x2_sem.at[2], x2_sem.at[3], d, flip(t, k))

    x2_all = rdma(xg.at[1:nt], xg.at[1:nt], x2_sem.at[0], x2_sem.at[1], mate, t)
    xp2_all = rdma(xp.at[1:nt], xp.at[1:nt], x2_sem.at[2], x2_sem.at[3], mate, t)

    def term_copy(k):
        return rdma(term.at[k * m:(k + 1) * m], termr.at[k], term_sem.at[0], term_sem.at[1], d, flip(t, k))

    term_out = rdma(term.at[m:g], term.at[m:g], term_sem.at[0], term_sem.at[1], mate, t)
    term_in = rdma(termr.at[1:nt], termr.at[1:nt], term_sem.at[0], term_sem.at[1], mate, t)

    def replica(c, chip, cr):
        return gall.at[c, rows_of(chip * CORES + cr, g)]

    def block(c, part, chip, cr):
        start = pl.multiple_of((chip * CORES + cr) * g, g) + (m if part else 0)
        return gall.at[c, pl.ds(pl.multiple_of(start, m), g - m if part else m)]

    def to_near(c, part):
        b = block(c, part, z, core)
        return rdma(b, b, zs.at[0], zr_near.at[c], near * CORES + core, t)

    def to_across(c, part):
        b = block(c, part, z, core)
        return rdma(b, b, zs.at[1], zr_rest.at[part, c], across * CORES + core, t)

    def near_in(c):
        b = replica(c, near, core)
        rdma(b, b, zs.at[0], zr_near.at[c], near * CORES + core, t).wait_recv()

    def rest_in(c, part):
        b = gall.at[c, 0:2 * (g - m if part else m)]
        rdma(b, b, zs.at[0], zr_rest.at[part, c], near * CORES + core, t).wait_recv()

    def forward(c, part):
        for chip in (across, far):
            b = block(c, part, chip, core)
            rdma(b, b, fs.at[0], zr_rest.at[part, c], near * CORES + core, t).start()

    def mate_copy(c, chip):
        b = replica(c, chip, core)
        if chip is near:
            return rdma(b, b, ms.at[1], mr_near.at[c], mate, t)
        return rdma(b, b, ms.at[0 if chip is z else 1], mr_rest.at[c], mate, t)

    def mate_near_in(c):
        b = gall.at[c, 0:g]
        rdma(b, b, ms.at[0], mr_near.at[c], mate, t).wait_recv()

    def mate_rest_in(c, replicas):
        b = gall.at[c, 0:replicas * g]
        rdma(b, b, ms.at[0], mr_rest.at[c], mate, t).wait_recv()

    def part_copy(j):
        return rdma(part_s.at[j], part_r.at[j], rs.at[0], rr.at[j], served, t)

    def grads(c, part):
        here = slice(m, g) if part else slice(0, m)
        cols = rows_of(c, hc)
        gate_pre = jnp.dot(tg[here], wv[c], preferred_element_type=F32)
        ug, gg = activation_grads(gate_pre, cotv[here, cols], upv[here, cols])
        start = pl.multiple_of(d * g, g) + (m if part else 0)
        gall[c, pl.ds(pl.multiple_of(start, m), g - m if part else m), :] = gg
        for k in range(1, nt) if part else (0,):
            low = (k - 1) * m if part else 0
            up_grad[rows_of(flip(t, k), m), cols] = ug[low:low + m]

    def send_own(c, part):
        to_across(c, part).start()

        @pl.when(jnp.logical_or(outer == 1, c < ng))
        def _():
            to_near(c, part).start()
        if part:
            mate_copy(c, z).start()

    span = dw // nc

    def term_part(n):
        rows = rows_of(n, span)
        own = rows_of(d, g)
        total = jnp.zeros((g, span), F32)
        for c in range(nc):
            total += lax.dot_general(
                gall[c, own, :], wv[c, rows, :], (((1,), (1,)), ((), ())), preferred_element_type=F32)
        term[:, rows] = total.astype(BF16)

    def step(c, grad):
        cols = rows_of(c, hc)
        first, second, change = adam(grad * scale, m1v[:, cols], m2v[:, cols])
        nm1[:, cols] = first.astype(BF16)
        nm2[:, cols] = second.astype(BF16)
        upd[:, cols] = change

    def update(c, reduced=False):
        mate_near_in(c)
        if not reduced:
            mate_rest_in(c, 3)
        step(c, jnp.dot(xt[...], gall[c], preferred_element_type=F32))

    def reduce(c, j):
        mate_rest_in(c, 3)
        rows = pl.ds(pl.multiple_of(first_rep * g, g), others * g)
        part_s[j] = jnp.dot(xtp[...], gall[c, rows, :], preferred_element_type=F32).astype(BF16)
        part_copy(j).start()

    def finish(c, j):
        mate_rest_in(c, 1)
        own = rows_of(z, CORES * g)
        grad = jnp.dot(xt[:, own], gall[c, own, :], preferred_element_type=F32)
        part_copy(j).wait_recv()
        step(c, grad + part_r[j].astype(F32))

    depth = min(W_DEPTH, nc)

    load_tok.start()
    barrier = pltpu.get_barrier_semaphore()

    def greet(dp, tn):
        pl.semaphore_signal(barrier, inc=1, device_id=(dp, tn), device_id_type=MESH)

    for k in range(1, nt):
        greet(d, flip(t, k))
    greet(mate, t)
    for cr in range(CORES):
        greet(near * CORES + cr, t)

    @inner_only
    def _():
        for chip in (across, far):
            for cr in range(CORES):
                greet(chip * CORES + cr, t)

    @phase
    def tok_load():
        load_tok.wait()

    for copy in cu_loads(0):
        copy.start()
    for c in range(depth):
        w_load(c).start()

    @phase
    def meet():
        pl.semaphore_wait(barrier, nt - 1 + 1 + 2 * CORES)

    for k in range(1, nt):
        tok_copy(k).start()

    @phase
    def own_loads():
        cu_wait(True)

    @phase
    def own_grads():
        @pl.loop(0, nc)
        def _(c):
            w_load(c).wait()

            @pl.when(c + depth < nc)
            def _():
                w_load(c + depth).start()
            grads(c, 0)

            @pl.when(jnp.logical_and(c > 0, c <= ng))
            def _():
                send_own(c - 1, 0)

    for k in range(1, nt):
        for copy in cu_loads(k):
            copy.start()
    load_x.start()
    inner_only(load_xp.start)
    load_m1.start()
    load_m2.start()
    for cr in range(CORES):
        xp_across(cr).start()
    for cr in range(CORES):
        x_across(cr).start()
        x_near(cr).start()
    x_mate.start()
    inner_only(xp_mate.start)

    @pl.loop(ng, nc)
    def _(c):
        send_own(c, 0)

    @phase
    def inner_forwards():
        @inner_only
        def _():
            @pl.loop(0, ng)
            def _(c):
                rest_in(c, 0)
                forward(c, 0)

    @phase
    def tok_wait():
        cu_wait(False)
        tok_all.wait_recv()

    @phase
    def other_grads():
        @pl.loop(0, nc)
        def _(c):
            grads(c, 1)

            @pl.when(c > 0)
            def _():
                send_own(c - 1, 1)

    @phase
    def x_exchange():
        term_part(0)
        send_own(nc - 1, 1)
        load_x.wait()

        @inner_only
        def _():
            xp_beyond.wait_recv()
            x_forward.start()
            load_xp.wait()
            xp_mate.wait_recv()
            x_all.wait_recv()
            for k in range(1, nt):
                x2_copy(k).start()
            for k in range(1, nt):
                xp2_copy(k).start()

    @phase
    def terms():
        @pl.loop(1, nc)
        def _(n):
            term_part(n)

    @phase
    def outer_x():
        @outer_only
        def _():
            x_all.wait_recv()
            for k in range(1, nt):
                x2_copy(k).start()
            for k in range(1, nt):
                term_copy(k).start()

    def takes(c):
        @phase
        def others_in():
            near_in(c)
            mate_copy(c, near).start()

            @outer_only
            def _():
                rest_in(c, 0)
            rest_in(c, 1)

            @inner_only
            def _():
                forward(c, 1)
            mate_copy(c, across).start()
            mate_copy(c, far).start()

    @pl.loop(0, lead)
    def _(c):
        takes(c)

    @inner_only
    def _():
        for k in range(1, nt):
            term_copy(k).start()

    @phase
    def x_wait():
        x2_all.wait_recv()

    load_m1.wait()
    load_m2.wait()

    @phase
    def transposes():
        for i in range(ndp):
            xt[:, i * g:(i + 1) * g] = xg[:, i].reshape(g, rw).T

    @pl.loop(lead, ng)
    def _(c):
        takes(c)

        @phase
        def updates():
            update(c - lead)

    def input_grads():
        with jax.named_scope("input_grads"):
            total = term[0:m, :].astype(F32)
            term_in.wait_recv()
            for k in range(1, nt):
                total += termr[k].astype(F32)
            in_grad[...] = total.astype(BF16)

    @inner_only
    def _():
        @phase
        def xp_wait():
            xp2_all.wait_recv()
            for i in range(others):
                xtp[:, i * g:(i + 1) * g] = xp[:, i].reshape(g, rw).T

        for j in range(nr):
            @phase
            def last_in():
                rest_in(ng + j, 0)
                rest_in(ng + j, 1)
                mate_copy(ng + j, across).start()
                mate_copy(ng + j, far).start()

            @phase
            def updates():
                update(ng - lead + j)

            @phase
            def reduces():
                reduce(ng + j, j)

            @phase
            def near_last():
                near_in(ng + j)
                mate_copy(ng + j, near).start()

        @pl.loop(ng - lead + nr, ng)
        def _(c):
            update(c)

        @pl.loop(ng, nc)
        def _(c):
            update(c, True)
        input_grads()

    @outer_only
    def _():
        @pl.loop(ng - lead, ng)
        def _(c):
            @phase
            def updates():
                update(c)
        input_grads()
        for j in range(nr):
            @phase
            def finishes():
                finish(ng + j, j)

    def sent(sem, chunks, replicas):
        b = gall.at[0:chunks, 0:replicas * g]
        rdma(b, b, sem, sem, mate, t).wait_send()

    @phase
    def drain():
        tok_all.wait_send()
        x2_all.wait_send()
        term_out.wait_send()
        x_all.wait_send()
        sent(zs.at[1], nc, 1)
        sent(ms.at[0], nc, 1)

        @outer_only
        def _():
            sent(zs.at[0], nc, 1)
            sent(ms.at[1], ng, 3)

        @inner_only
        def _():
            sent(zs.at[0], ng, 1)
            sent(ms.at[1], nc, 3)
            sent(fs.at[0], ng, 2)
            xp_mate.wait_send()
            x_forward.wait_send()
            xp2_all.wait_send()
            rdma(part_s, part_s, rs.at[0], rs.at[0], mate, t).wait_send()


def fused(ndp, nt, tokens, gate_weight, up_act, cotangent, moment1, moment2):
    m, dw = tokens.shape
    g, hid = up_act.shape
    rw = moment1.shape[0]
    nc = hid // WIDE
    nr = SUMMED * nc // 8
    any_spec, vmem = pl.BlockSpec(memory_space=pltpu.HBM), pl.BlockSpec(memory_space=pltpu.VMEM)
    dma = pltpu.SemaphoreType.DMA
    results = (((m, dw), BF16), ((g, hid), BF16), ((rw, hid), BF16), ((rw, hid), BF16), ((rw, hid), F32))
    held = pl.pallas_call(
        functools.partial(kernel, ndp, nt),
        out_shape=tuple(pltpu.VMEM(shape, dtype) for shape, dtype in results),
        in_specs=[any_spec] * 6,
        out_specs=(vmem,) * 5,
        scratch_shapes=[
            pltpu.VMEM((g, dw), BF16),
            pltpu.VMEM((nt, ndp, m, rw), BF16),
            pltpu.VMEM((nt, ndp - CORES, m, rw), BF16),
            pltpu.VMEM((rw, ndp * g), BF16),
            pltpu.VMEM((rw, (ndp - CORES) * g), BF16),
            pltpu.VMEM((nc, dw, WIDE), BF16),
            pltpu.VMEM((g, hid), BF16),
            pltpu.VMEM((g, hid), BF16),
            pltpu.VMEM((rw, hid), BF16),
            pltpu.VMEM((rw, hid), BF16),
            pltpu.VMEM((nc, ndp * g, WIDE), BF16),
            pltpu.VMEM((g, dw), BF16),
            pltpu.VMEM((nt, m, dw), BF16),
            pltpu.VMEM((nr, rw, WIDE), BF16),
            pltpu.VMEM((nr, rw, WIDE), BF16),
            dma((5,)), dma((nc,)), dma((3,)), dma((2,)), dma((6,)), dma((4,)),
            dma((2,)), dma((1,)), dma((2,)), dma((nc,)), dma((2, nc)),
            dma((nc,)), dma((nc,)), dma((1,)), dma((nr,)), dma((2,)),
        ],
        compiler_params=pltpu.CompilerParams(
            collective_id=0, has_side_effects=True, vmem_limit_bytes=VMEM_BUDGET),
    )(*(pltpu.with_memory_space_constraint(x, pltpu.HBM)
        for x in (tokens, gate_weight, up_act, cotangent, moment1, moment2)))
    return pl.pallas_call(
        write_out,
        out_shape=tuple(pltpu.HBM(shape, dtype) for shape, dtype in results),
        in_specs=[vmem] * 5,
        out_specs=(any_spec,) * 5,
        scratch_shapes=[dma((5,))],
        compiler_params=pltpu.CompilerParams(vmem_limit_bytes=2**20),
    )(*(pltpu.with_memory_space_constraint(x, pltpu.VMEM) for x in held))


def write_out(*refs):
    sems = refs[-1]
    copies = [pltpu.make_async_copy(refs[i], refs[5 + i], sems.at[i]) for i in range(5)]
    for copy in reversed(copies):
        copy.start()
    for copy in copies:
        copy.wait()


def plain(ndp, nt, tokens, gate_weight, up_act, cotangent, moment1, moment2):
    gathered = lax.all_gather(tokens, "tensor", axis=0, tiled=True)
    gate_pre = jnp.dot(gathered, gate_weight, preferred_element_type=F32)
    up_grad, gate_grad = activation_grads(gate_pre, cotangent, up_act)
    term = lax.dot_general(
        gate_grad, gate_weight, (((1,), (1,)), ((), ())), preferred_element_type=F32).astype(BF16)
    in_grad = lax.psum_scatter(term, "tensor", scatter_dimension=0, tiled=True)
    partial_value = lax.dot_general(
        gathered, gate_grad, (((0,), (0,)), ((), ())), preferred_element_type=F32).astype(BF16)
    shard = lax.psum_scatter(partial_value.astype(F32), "dp", scatter_dimension=0, tiled=True)
    first, second, update = adam(shard * (1.0 / math.sqrt(ndp * gathered.shape[0])), moment1, moment2)
    return in_grad, up_grad, first.astype(BF16), second.astype(BF16), update


def local(ndp, nt, *args):
    (m, dw), (g, hid), rw = args[0].shape, args[2].shape, args[4].shape[0]
    need = (2 * dw * hid + 2 * ndp * g * (hid + 2 * rw) + 12 * g * hid + 16 * rw * hid + 16 * g * dw)
    fits = (need <= VMEM_BUDGET and hid >= 8 * WIDE and ndp == CORES * CHIPS and nt > 1 and nt & (nt - 1) == 0
            and hid % WIDE == 0 and g % 128 == 0 and rw % 128 == 0 and m % 16 == 0
            and dw % (128 * (hid // WIDE)) == 0)
    return (fused if fits else plain)(ndp, nt, *args)


def solution(mesh):
    both = P("dp", "tensor")
    rows = P(("dp", "tensor"), None)
    return jax.shard_map(
        functools.partial(local, mesh.shape["dp"], mesh.shape["tensor"]),
        mesh=mesh,
        in_specs=(rows, P(None, "tensor"), both, both, both, both),
        out_specs=(rows, both, both, both, both),
        check_vma=False,
    )
```

```python
import functools
import math

import jax
import jax.numpy as jnp
from jax import lax
from jax.experimental import pallas as pl
from jax.experimental.pallas import tpu as pltpu
from jax.sharding import PartitionSpec as P

MESH = pl.DeviceIdType.MESH
F32, BF16 = jnp.float32, jnp.bfloat16
CORES = 2
CHIPS = 4
WIDE = 256
SUMMED = 2
LEAD = 4
W_DEPTH = 3
EARLY = 3
EARLY_LAG = 2
VMEM_BUDGET = 48 * 2**20


def adam(grad, moment1, moment2):
    first = 0.9 * moment1.astype(F32) + 0.1 * grad
    second = 0.95 * moment2.astype(F32) + 0.05 * grad * grad
    return first, second, first / (jnp.sqrt(second) + 1e-08)


def activation_grads(gate_pre, cot, up):
    sig = jax.nn.sigmoid(gate_pre)
    cot = cot.astype(F32)
    up_grad = (cot * gate_pre * sig).astype(BF16)
    gate_grad = (cot * up.astype(F32) * sig * (1.0 + gate_pre * (1.0 - sig))).astype(BF16)
    return up_grad, gate_grad


def phase(run):
    with jax.named_scope(run.__name__):
        run()


def flip(t, k):
    bit = 1
    while bit <= k:
        if k & bit:
            t = t + bit - 2 * bit * lax.rem(t // bit, 2)
        bit *= 2
    return t


def kernel(ndp, nt, tok, w, up, cot, m1, m2, in_grad, up_grad, nm1, nm2, upd,
           tg, xg, xp, xt, xtp, wv, upv, cotv, m1v, m2v, gall, term, termr, part_s, part_r,
           loc_sem, w_sem, cu_sem, tok_sem, x_sem, x2_sem, zs, fs, ms, zr_near, zr_rest,
           mr_near, mr_rest, rs, rr, term_sem):
    d, t = lax.axis_index("dp"), lax.axis_index("tensor")
    z, core = d // CORES, lax.rem(d, CORES)
    mate = d + 1 - 2 * core
    m, dw = tok.shape
    g, hid = up.shape
    rw = m1.shape[0]
    nc, _, hc = wv.shape
    nr = part_s.shape[0]
    ng = nc - nr
    lead = min(LEAD, ng)
    early = (nt // 2 + 1) * m
    A, B, B_EARLY, B_LATE = (0, m), (m, g), (m, early), (early, g)
    ns = min(EARLY, ng - EARLY_LAG)
    scale = 1.0 / math.sqrt(ndp * g)

    half = z // 2
    near = z + 1 - 2 * lax.rem(z, 2)
    across = 2 - half
    far = 3 - 3 * half
    outer = lax.rem(z + half + 1, 2)
    first_rep = CORES * (1 - half)
    others = ndp - CORES
    beyond = others - CORES

    def inner_only(run):
        pl.when(outer == 0)(run)

    def outer_only(run):
        pl.when(outer == 1)(run)

    def rdma(src, dst, s, r, dp, tn):
        return pltpu.make_async_remote_copy(
            src_ref=src, dst_ref=dst, send_sem=s, recv_sem=r, device_id=(dp, tn), device_id_type=MESH)

    def rows_of(i, size):
        return pl.ds(pl.multiple_of(i * size, size), size)

    served = near * CORES + 1 - core

    load_tok = pltpu.make_async_copy(tok, tg.at[0:m], loc_sem.at[0])
    load_x = pltpu.make_async_copy(tok.at[:, rows_of(d, rw)], xg.at[0, d], loc_sem.at[1])
    load_xp = pltpu.make_async_copy(tok.at[:, rows_of(served, rw)], xp.at[0, d - first_rep], loc_sem.at[4])
    load_m1 = pltpu.make_async_copy(m1, m1v, loc_sem.at[2])
    load_m2 = pltpu.make_async_copy(m2, m2v, loc_sem.at[3])

    def w_load(c):
        return pltpu.make_async_copy(w.at[:, rows_of(c, hc)], wv.at[c], w_sem.at[c])

    def cu_loads(k):
        src = rows_of(flip(t, k), m)
        dst = pl.ds(k * m, m)
        return (pltpu.make_async_copy(cot.at[src], cotv.at[dst], cu_sem.at[1 if k else 0]),
                pltpu.make_async_copy(up.at[src], upv.at[dst], cu_sem.at[2 if k else 0]))

    def cu_wait(first):
        if first:
            pltpu.make_async_copy(cot.at[0:2 * m], cotv.at[0:2 * m], cu_sem.at[0]).wait()
        else:
            pltpu.make_async_copy(cot.at[m:g], cotv.at[m:g], cu_sem.at[1]).wait()
            pltpu.make_async_copy(up.at[m:g], upv.at[m:g], cu_sem.at[2]).wait()

    def tok_copy(k):
        return rdma(tg.at[0:m], tg.at[k * m:(k + 1) * m], tok_sem.at[0],
                    tok_sem.at[1 if k * m < early else 2], d, flip(t, k))

    tok_all = rdma(tg.at[m:g], tg.at[m:g], tok_sem.at[0], tok_sem.at[1], mate, t)
    tok_early = rdma(tg.at[m:early], tg.at[m:early], tok_sem.at[0], tok_sem.at[1], mate, t)
    tok_late = rdma(tg.at[early:g], tg.at[early:g], tok_sem.at[0], tok_sem.at[2], mate, t)

    def features(chip, cr):
        return tg.at[0:m, rows_of(chip * CORES + cr, rw)]

    def x_near(cr):
        return rdma(features(near, cr), xg.at[0, d], x_sem.at[0], x_sem.at[1], near * CORES + cr, t)

    def x_across(cr):
        return rdma(features(across, cr), xg.at[0, d], x_sem.at[0], x_sem.at[1], across * CORES + cr, t)

    def xp_across(cr):
        return rdma(features(far, 1 - cr), xp.at[0, d - CORES * half], x_sem.at[0], x_sem.at[2],
                    across * CORES + cr, t)

    x_mate = rdma(features(z, 1 - core), xg.at[0, d], x_sem.at[0], x_sem.at[1], mate, t)
    xp_mate = rdma(features(near, core), xp.at[0, d - first_rep], x_sem.at[3], x_sem.at[4], mate, t)
    x_forward = rdma(xp.at[0, pl.ds(first_rep, beyond)], xg.at[0, pl.ds(CORES * first_rep, beyond)],
                     x_sem.at[5], x_sem.at[1], served, t)
    x_all = rdma(xg.at[0, 0:ndp - 1], xg.at[0, 0:ndp - 1], x_sem.at[0], x_sem.at[1], mate, t)
    xp_beyond = rdma(xp.at[0, 0:beyond], xp.at[0, 0:beyond], x_sem.at[5], x_sem.at[2], mate, t)

    def x2_copy(k):
        return rdma(xg.at[0], xg.at[k], x2_sem.at[0], x2_sem.at[1], d, flip(t, k))

    def xp2_copy(k):
        return rdma(xp.at[0], xp.at[k], x2_sem.at[2], x2_sem.at[3], d, flip(t, k))

    x2_all = rdma(xg.at[1:nt], xg.at[1:nt], x2_sem.at[0], x2_sem.at[1], mate, t)
    xp2_all = rdma(xp.at[1:nt], xp.at[1:nt], x2_sem.at[2], x2_sem.at[3], mate, t)

    def term_copy(k):
        return rdma(term.at[k * m:(k + 1) * m], termr.at[k], term_sem.at[0], term_sem.at[1], d, flip(t, k))

    term_out = rdma(term.at[m:g], term.at[m:g], term_sem.at[0], term_sem.at[1], mate, t)
    term_in = rdma(termr.at[1:nt], termr.at[1:nt], term_sem.at[0], term_sem.at[1], mate, t)

    def replica(c, chip, cr):
        return gall.at[c, rows_of(chip * CORES + cr, g)]

    def span_of(index, rows):
        return pl.ds(pl.multiple_of(index * g + rows[0], m), rows[1] - rows[0])

    def block(c, rows, chip):
        return gall.at[c, span_of(chip * CORES + core, rows)]

    def to_near(c, rows):
        b = block(c, rows, z)
        return rdma(b, b, zs.at[0], zr_near.at[c], near * CORES + core, t)

    def to_across(c, rows):
        b = block(c, rows, z)
        return rdma(b, b, zs.at[1], zr_rest.at[0 if rows == A else 1, c], across * CORES + core, t)

    def near_in(c):
        b = replica(c, near, core)
        rdma(b, b, zs.at[0], zr_near.at[c], near * CORES + core, t).wait_recv()

    def rest_in(c, rows):
        b = gall.at[c, 0:2 * (rows[1] - rows[0])]
        rdma(b, b, zs.at[0], zr_rest.at[0 if rows == A else 1, c], near * CORES + core, t).wait_recv()

    def forward(c, rows):
        for chip in (across, far):
            b = block(c, rows, chip)
            rdma(b, b, fs.at[0], zr_rest.at[0 if rows == A else 1, c], near * CORES + core, t).start()

    def mate_copy(c, chip):
        b = replica(c, chip, core)
        if chip is near:
            return rdma(b, b, ms.at[1], mr_near.at[c], mate, t)
        return rdma(b, b, ms.at[0 if chip is z else 1], mr_rest.at[c], mate, t)

    def mate_near_in(c):
        b = gall.at[c, 0:g]
        rdma(b, b, ms.at[0], mr_near.at[c], mate, t).wait_recv()

    def mate_rest_in(c, replicas):
        b = gall.at[c, 0:replicas * g]
        rdma(b, b, ms.at[0], mr_rest.at[c], mate, t).wait_recv()

    def part_copy(j):
        return rdma(part_s.at[j], part_r.at[j], rs.at[0], rr.at[j], served, t)

    def grads(c, rows):
        here = slice(*rows)
        cols = rows_of(c, hc)
        gate_pre = jnp.dot(tg[here], wv[c], preferred_element_type=F32)
        ug, gg = activation_grads(gate_pre, cotv[here, cols], upv[here, cols])
        gall[c, span_of(d, rows), :] = gg
        for k in range(rows[0] // m, rows[1] // m):
            low = k * m - rows[0]
            up_grad[rows_of(flip(t, k), m), cols] = ug[low:low + m]

    def send_near(c, rows):
        @pl.when(jnp.logical_or(outer == 1, c < ng))
        def _():
            to_near(c, rows).start()

    def send_first(c):
        to_across(c, A).start()
        send_near(c, A)

    def send_rest(c, near_rows=B):
        send_near(c, near_rows)
        to_across(c, B).start()
        mate_copy(c, z).start()

    span = dw // nc

    def term_part(n):
        rows = rows_of(n, span)
        own = rows_of(d, g)
        total = jnp.zeros((g, span), F32)
        for c in range(nc):
            total += lax.dot_general(
                gall[c, own, :], wv[c, rows, :], (((1,), (1,)), ((), ())), preferred_element_type=F32)
        term[:, rows] = total.astype(BF16)

    def step(c, grad):
        cols = rows_of(c, hc)
        first, second, change = adam(grad * scale, m1v[:, cols], m2v[:, cols])
        nm1[:, cols] = first.astype(BF16)
        nm2[:, cols] = second.astype(BF16)
        upd[:, cols] = change

    def update(c, reduced=False):
        mate_near_in(c)
        if not reduced:
            mate_rest_in(c, 3)
        step(c, jnp.dot(xt[...], gall[c], preferred_element_type=F32))

    def reduce(c, j):
        mate_rest_in(c, 3)
        rows = pl.ds(pl.multiple_of(first_rep * g, g), others * g)
        part_s[j] = jnp.dot(xtp[...], gall[c, rows, :], preferred_element_type=F32).astype(BF16)
        part_copy(j).start()

    def finish(c, j):
        mate_rest_in(c, 1)
        own = rows_of(z, CORES * g)
        grad = jnp.dot(xt[:, own], gall[c, own, :], preferred_element_type=F32)
        part_copy(j).wait_recv()
        step(c, grad + part_r[j].astype(F32))

    depth = min(W_DEPTH, nc)

    load_tok.start()
    barrier = pltpu.get_barrier_semaphore()

    def greet(dp, tn):
        pl.semaphore_signal(barrier, inc=1, device_id=(dp, tn), device_id_type=MESH)

    for k in range(1, nt):
        greet(d, flip(t, k))
    greet(mate, t)
    for cr in range(CORES):
        greet(near * CORES + cr, t)

    @inner_only
    def _():
        for chip in (across, far):
            for cr in range(CORES):
                greet(chip * CORES + cr, t)

    @phase
    def tok_load():
        load_tok.wait()

    for copy in cu_loads(0):
        copy.start()
    for c in range(depth):
        w_load(c).start()

    @phase
    def meet():
        pl.semaphore_wait(barrier, nt - 1 + 1 + 2 * CORES)

    for k in range(1, nt):
        tok_copy(k).start()

    @phase
    def own_loads():
        cu_wait(True)

    @phase
    def own_grads():
        @pl.loop(0, nc)
        def _(c):
            w_load(c).wait()

            @pl.when(c + depth < nc)
            def _():
                w_load(c + depth).start()

            @pl.when(c == nc // 2)
            def _():
                for k in range(1, nt):
                    for copy in cu_loads(k):
                        copy.start()
            grads(c, A)

            @pl.when(jnp.logical_and(c > 0, c <= ng))
            def _():
                send_first(c - 1)

    load_x.start()
    inner_only(load_xp.start)
    load_m1.start()
    load_m2.start()
    for cr in range(CORES):
        xp_across(cr).start()
    for cr in range(CORES):
        x_across(cr).start()
        x_near(cr).start()
    x_mate.start()
    inner_only(xp_mate.start)

    @pl.loop(ng, nc)
    def _(c):
        send_first(c)

    @phase
    def inner_forwards():
        @inner_only
        def _():
            @pl.loop(0, EARLY_LAG)
            def _(c):
                rest_in(c, A)
                forward(c, A)
            cu_wait(False)
            tok_early.wait_recv()

            @pl.loop(0, ns)
            def _(c):
                grads(c, B_EARLY)
                rest_in(EARLY_LAG + c, A)
                forward(EARLY_LAG + c, A)
                to_near(c, B_EARLY).start()

            @pl.loop(EARLY_LAG + ns, ng)
            def _(c):
                rest_in(c, A)
                forward(c, A)

        @outer_only
        def _():
            cu_wait(False)
            tok_early.wait_recv()

    @phase
    def tok_wait():
        tok_late.wait_recv()

    @phase
    def other_grads():
        @inner_only
        def _():
            @pl.loop(0, ns)
            def _(c):
                grads(c, B_LATE)

                @pl.when(c > 0)
                def _():
                    send_rest(c - 1, B_LATE)
            grads(ns, B)
            send_rest(ns - 1, B_LATE)

        @outer_only
        def _():
            @pl.loop(0, ns + 1)
            def _(c):
                grads(c, B)

                @pl.when(c > 0)
                def _():
                    send_rest(c - 1)

        @pl.loop(ns + 1, nc)
        def _(c):
            grads(c, B)
            send_rest(c - 1)

    @phase
    def x_exchange():
        term_part(0)
        send_rest(nc - 1)
        load_x.wait()

        @inner_only
        def _():
            xp_beyond.wait_recv()
            x_forward.start()
            load_xp.wait()
            xp_mate.wait_recv()
            x_all.wait_recv()
            for k in range(1, nt):
                x2_copy(k).start()
            for k in range(1, nt):
                xp2_copy(k).start()

    @phase
    def terms():
        @pl.loop(1, nc)
        def _(n):
            term_part(n)

    @phase
    def outer_x():
        @outer_only
        def _():
            x_all.wait_recv()
            for k in range(1, nt):
                x2_copy(k).start()
            for k in range(1, nt):
                term_copy(k).start()

    def takes(c):
        @phase
        def others_in():
            near_in(c)
            mate_copy(c, near).start()

            @outer_only
            def _():
                rest_in(c, A)
            rest_in(c, B)

            @inner_only
            def _():
                forward(c, B)
            mate_copy(c, across).start()
            mate_copy(c, far).start()

    @pl.loop(0, lead)
    def _(c):
        takes(c)

    @inner_only
    def _():
        for k in range(1, nt):
            term_copy(k).start()

    @phase
    def x_wait():
        x2_all.wait_recv()

    load_m1.wait()
    load_m2.wait()

    @phase
    def transposes():
        for i in range(ndp):
            xt[:, i * g:(i + 1) * g] = xg[:, i].reshape(g, rw).T

    @pl.loop(lead, ng)
    def _(c):
        takes(c)

        @phase
        def updates():
            update(c - lead)

    def input_grads():
        with jax.named_scope("input_grads"):
            total = term[0:m, :].astype(F32)
            term_in.wait_recv()
            for k in range(1, nt):
                total += termr[k].astype(F32)
            in_grad[...] = total.astype(BF16)

    @inner_only
    def _():
        @phase
        def xp_wait():
            xp2_all.wait_recv()
            for i in range(others):
                xtp[:, i * g:(i + 1) * g] = xp[:, i].reshape(g, rw).T

        for j in range(nr):
            @phase
            def last_in():
                rest_in(ng + j, A)
                rest_in(ng + j, B)
                mate_copy(ng + j, across).start()
                mate_copy(ng + j, far).start()

            @phase
            def updates():
                update(ng - lead + j)

            @phase
            def reduces():
                reduce(ng + j, j)

            @phase
            def near_last():
                near_in(ng + j)
                mate_copy(ng + j, near).start()

        @pl.loop(ng - lead + nr, ng)
        def _(c):
            update(c)

        @pl.loop(ng, nc)
        def _(c):
            update(c, True)
        input_grads()

    @outer_only
    def _():
        @pl.loop(ng - lead, ng)
        def _(c):
            @phase
            def updates():
                update(c)
        input_grads()
        for j in range(nr):
            @phase
            def finishes():
                finish(ng + j, j)

    def sent(sem, chunks, replicas):
        b = gall.at[0:chunks, 0:replicas * g]
        rdma(b, b, sem, sem, mate, t).wait_send()

    @phase
    def drain():
        tok_all.wait_send()
        x2_all.wait_send()
        term_out.wait_send()
        x_all.wait_send()
        sent(zs.at[1], nc, 1)
        sent(ms.at[0], nc, 1)

        @outer_only
        def _():
            sent(zs.at[0], nc, 1)
            sent(ms.at[1], ng, 3)

        @inner_only
        def _():
            sent(zs.at[0], ng, 1)
            sent(ms.at[1], nc, 3)
            sent(fs.at[0], ng, 2)
            xp_mate.wait_send()
            x_forward.wait_send()
            xp2_all.wait_send()
            rdma(part_s, part_s, rs.at[0], rs.at[0], mate, t).wait_send()


def fused(ndp, nt, tokens, gate_weight, up_act, cotangent, moment1, moment2):
    m, dw = tokens.shape
    g, hid = up_act.shape
    rw = moment1.shape[0]
    nc = hid // WIDE
    nr = SUMMED * nc // 8
    any_spec, vmem = pl.BlockSpec(memory_space=pltpu.HBM), pl.BlockSpec(memory_space=pltpu.VMEM)
    dma = pltpu.SemaphoreType.DMA
    results = (((m, dw), BF16), ((g, hid), BF16), ((rw, hid), BF16), ((rw, hid), BF16), ((rw, hid), F32))
    held = pl.pallas_call(
        functools.partial(kernel, ndp, nt),
        out_shape=tuple(pltpu.VMEM(shape, dtype) for shape, dtype in results),
        in_specs=[any_spec] * 6,
        out_specs=(vmem,) * 5,
        scratch_shapes=[
            pltpu.VMEM((g, dw), BF16),
            pltpu.VMEM((nt, ndp, m, rw), BF16),
            pltpu.VMEM((nt, ndp - CORES, m, rw), BF16),
            pltpu.VMEM((rw, ndp * g), BF16),
            pltpu.VMEM((rw, (ndp - CORES) * g), BF16),
            pltpu.VMEM((nc, dw, WIDE), BF16),
            pltpu.VMEM((g, hid), BF16),
            pltpu.VMEM((g, hid), BF16),
            pltpu.VMEM((rw, hid), BF16),
            pltpu.VMEM((rw, hid), BF16),
            pltpu.VMEM((nc, ndp * g, WIDE), BF16),
            pltpu.VMEM((g, dw), BF16),
            pltpu.VMEM((nt, m, dw), BF16),
            pltpu.VMEM((nr, rw, WIDE), BF16),
            pltpu.VMEM((nr, rw, WIDE), BF16),
            dma((5,)), dma((nc,)), dma((3,)), dma((3,)), dma((6,)), dma((4,)),
            dma((2,)), dma((1,)), dma((2,)), dma((nc,)), dma((2, nc)),
            dma((nc,)), dma((nc,)), dma((1,)), dma((nr,)), dma((2,)),
        ],
        compiler_params=pltpu.CompilerParams(
            collective_id=0, has_side_effects=True, vmem_limit_bytes=VMEM_BUDGET),
    )(*(pltpu.with_memory_space_constraint(x, pltpu.HBM)
        for x in (tokens, gate_weight, up_act, cotangent, moment1, moment2)))
    return pl.pallas_call(
        write_out,
        out_shape=tuple(pltpu.HBM(shape, dtype) for shape, dtype in results),
        in_specs=[vmem] * 5,
        out_specs=(any_spec,) * 5,
        scratch_shapes=[dma((5,))],
        compiler_params=pltpu.CompilerParams(vmem_limit_bytes=2**20),
    )(*(pltpu.with_memory_space_constraint(x, pltpu.VMEM) for x in held))


def write_out(*refs):
    sems = refs[-1]
    copies = [pltpu.make_async_copy(refs[i], refs[5 + i], sems.at[i]) for i in range(5)]
    for copy in reversed(copies):
        copy.start()
    for copy in copies:
        copy.wait()


def plain(ndp, nt, tokens, gate_weight, up_act, cotangent, moment1, moment2):
    gathered = lax.all_gather(tokens, "tensor", axis=0, tiled=True)
    gate_pre = jnp.dot(gathered, gate_weight, preferred_element_type=F32)
    up_grad, gate_grad = activation_grads(gate_pre, cotangent, up_act)
    term = lax.dot_general(
        gate_grad, gate_weight, (((1,), (1,)), ((), ())), preferred_element_type=F32).astype(BF16)
    in_grad = lax.psum_scatter(term, "tensor", scatter_dimension=0, tiled=True)
    partial_value = lax.dot_general(
        gathered, gate_grad, (((0,), (0,)), ((), ())), preferred_element_type=F32).astype(BF16)
    shard = lax.psum_scatter(partial_value.astype(F32), "dp", scatter_dimension=0, tiled=True)
    first, second, update = adam(shard * (1.0 / math.sqrt(ndp * gathered.shape[0])), moment1, moment2)
    return in_grad, up_grad, first.astype(BF16), second.astype(BF16), update


def local(ndp, nt, *args):
    (m, dw), (g, hid), rw = args[0].shape, args[2].shape, args[4].shape[0]
    need = (2 * dw * hid + 2 * ndp * g * (hid + 2 * rw) + 12 * g * hid + 16 * rw * hid + 16 * g * dw)
    fits = (need <= VMEM_BUDGET and hid >= 8 * WIDE and ndp == CORES * CHIPS and nt > 1 and nt & (nt - 1) == 0
            and hid % WIDE == 0 and g % 128 == 0 and rw % 128 == 0 and m % 16 == 0
            and dw % (128 * (hid // WIDE)) == 0)
    return (fused if fits else plain)(ndp, nt, *args)


def solution(mesh):
    both = P("dp", "tensor")
    rows = P(("dp", "tensor"), None)
    return jax.shard_map(
        functools.partial(local, mesh.shape["dp"], mesh.shape["tensor"]),
        mesh=mesh,
        in_specs=(rows, P(None, "tensor"), both, both, both, both),
        out_specs=(rows, both, both, both, both),
        check_vma=False,
    )
```

```python
import functools
import math

import jax
import jax.numpy as jnp
from jax import lax
from jax.experimental import pallas as pl
from jax.experimental.pallas import tpu as pltpu
from jax.sharding import PartitionSpec as P

MESH = pl.DeviceIdType.MESH
F32, BF16 = jnp.float32, jnp.bfloat16
CORES = 2
CHIPS = 4
WIDE = 256
SUMMED = 2
LEAD = 4
W_DEPTH = 3
ALONE = 3
EARLY = 3
EARLY_LAG = 2
VMEM_BUDGET = 48 * 2**20


def adam(grad, moment1, moment2):
    first = 0.9 * moment1.astype(F32) + 0.1 * grad
    second = 0.95 * moment2.astype(F32) + 0.05 * grad * grad
    return first, second, first / (jnp.sqrt(second) + 1e-08)


def activation_grads(gate_pre, cot, up):
    sig = jax.nn.sigmoid(gate_pre)
    cot = cot.astype(F32)
    up_grad = (cot * gate_pre * sig).astype(BF16)
    gate_grad = (cot * up.astype(F32) * sig * (1.0 + gate_pre * (1.0 - sig))).astype(BF16)
    return up_grad, gate_grad


def phase(run):
    with jax.named_scope(run.__name__):
        run()


def flip(t, k):
    bit = 1
    while bit <= k:
        if k & bit:
            t = t + bit - 2 * bit * lax.rem(t // bit, 2)
        bit *= 2
    return t


def kernel(ndp, nt, tok, w, up, cot, m1, m2, in_grad, up_grad, nm1, nm2, upd,
           tg, xg, xp, xt, xtp, wv, upv, cotv, m1v, m2v, gall, term, termr, part_s, part_r,
           loc_sem, w_sem, cu_sem, tok_sem, x_sem, x2_sem, zs, fs, ms, zr_near, zr_rest,
           mr_near, mr_rest, rs, rr, term_sem, go):
    d, t = lax.axis_index("dp"), lax.axis_index("tensor")
    z, core = d // CORES, lax.rem(d, CORES)
    mate = d + 1 - 2 * core
    m, dw = tok.shape
    g, hid = up.shape
    rw = m1.shape[0]
    nc, _, hc = wv.shape
    nr = part_s.shape[0]
    ng = nc - nr
    lead = min(LEAD, ng)
    early = (nt // 2 + 1) * m
    A, B, B_EARLY, B_LATE = (0, m), (m, g), (m, early), (early, g)
    ns = min(EARLY, ng - EARLY_LAG)
    scale = 1.0 / math.sqrt(ndp * g)

    half = z // 2
    near = z + 1 - 2 * lax.rem(z, 2)
    across = 2 - half
    far = 3 - 3 * half
    outer = lax.rem(z + half + 1, 2)
    first_rep = CORES * (1 - half)
    others = ndp - CORES
    beyond = others - CORES

    def inner_only(run):
        pl.when(outer == 0)(run)

    def outer_only(run):
        pl.when(outer == 1)(run)

    def rdma(src, dst, s, r, dp, tn):
        return pltpu.make_async_remote_copy(
            src_ref=src, dst_ref=dst, send_sem=s, recv_sem=r, device_id=(dp, tn), device_id_type=MESH)

    def rows_of(i, size):
        return pl.ds(pl.multiple_of(i * size, size), size)

    served = near * CORES + 1 - core

    load_tok = pltpu.make_async_copy(tok, tg.at[0:m], loc_sem.at[0])
    load_x = pltpu.make_async_copy(tok.at[:, rows_of(d, rw)], xg.at[0, d], loc_sem.at[1])
    load_xp = pltpu.make_async_copy(tok.at[:, rows_of(served, rw)], xp.at[0, d - first_rep], loc_sem.at[4])
    load_m1 = pltpu.make_async_copy(m1, m1v, loc_sem.at[2])
    load_m2 = pltpu.make_async_copy(m2, m2v, loc_sem.at[3])

    def w_load(c):
        return pltpu.make_async_copy(w.at[:, rows_of(c, hc)], wv.at[c], w_sem.at[c])

    def cu_loads(k):
        src = rows_of(flip(t, k), m)
        dst = pl.ds(k * m, m)
        return (pltpu.make_async_copy(cot.at[src], cotv.at[dst], cu_sem.at[1 if k else 0]),
                pltpu.make_async_copy(up.at[src], upv.at[dst], cu_sem.at[2 if k else 0]))

    def cu_wait(first):
        if first:
            pltpu.make_async_copy(cot.at[0:2 * m], cotv.at[0:2 * m], cu_sem.at[0]).wait()
        else:
            pltpu.make_async_copy(cot.at[m:g], cotv.at[m:g], cu_sem.at[1]).wait()
            pltpu.make_async_copy(up.at[m:g], upv.at[m:g], cu_sem.at[2]).wait()

    def tok_copy(k):
        return rdma(tg.at[0:m], tg.at[k * m:(k + 1) * m], tok_sem.at[0],
                    tok_sem.at[1 if k * m < early else 2], d, flip(t, k))

    tok_all = rdma(tg.at[m:g], tg.at[m:g], tok_sem.at[0], tok_sem.at[1], mate, t)
    tok_early = rdma(tg.at[m:early], tg.at[m:early], tok_sem.at[0], tok_sem.at[1], mate, t)
    tok_late = rdma(tg.at[early:g], tg.at[early:g], tok_sem.at[0], tok_sem.at[2], mate, t)

    def features(chip, cr):
        return tg.at[0:m, rows_of(chip * CORES + cr, rw)]

    def x_near(cr):
        return rdma(features(near, cr), xg.at[0, d], x_sem.at[0], x_sem.at[1], near * CORES + cr, t)

    def x_across(cr):
        return rdma(features(across, cr), xg.at[0, d], x_sem.at[0], x_sem.at[1], across * CORES + cr, t)

    def xp_across(cr):
        return rdma(features(far, 1 - cr), xp.at[0, d - CORES * half], x_sem.at[0], x_sem.at[2],
                    across * CORES + cr, t)

    x_mate = rdma(features(z, 1 - core), xg.at[0, d], x_sem.at[0], x_sem.at[1], mate, t)
    xp_mate = rdma(features(near, core), xp.at[0, d - first_rep], x_sem.at[3], x_sem.at[4], mate, t)
    x_forward = rdma(xp.at[0, pl.ds(first_rep, beyond)], xg.at[0, pl.ds(CORES * first_rep, beyond)],
                     x_sem.at[5], x_sem.at[1], served, t)
    x_all = rdma(xg.at[0, 0:ndp - 1], xg.at[0, 0:ndp - 1], x_sem.at[0], x_sem.at[1], mate, t)
    xp_beyond = rdma(xp.at[0, 0:beyond], xp.at[0, 0:beyond], x_sem.at[5], x_sem.at[2], mate, t)

    def x2_copy(k):
        return rdma(xg.at[0], xg.at[k], x2_sem.at[0], x2_sem.at[1], d, flip(t, k))

    def xp2_copy(k):
        return rdma(xp.at[0], xp.at[k], x2_sem.at[2], x2_sem.at[3], d, flip(t, k))

    x2_all = rdma(xg.at[1:nt], xg.at[1:nt], x2_sem.at[0], x2_sem.at[1], mate, t)
    xp2_all = rdma(xp.at[1:nt], xp.at[1:nt], x2_sem.at[2], x2_sem.at[3], mate, t)

    def term_copy(k):
        return rdma(term.at[k * m:(k + 1) * m], termr.at[k], term_sem.at[0], term_sem.at[1], d, flip(t, k))

    term_out = rdma(term.at[m:g], term.at[m:g], term_sem.at[0], term_sem.at[1], mate, t)
    term_in = rdma(termr.at[1:nt], termr.at[1:nt], term_sem.at[0], term_sem.at[1], mate, t)

    def replica(c, chip, cr):
        return gall.at[c, rows_of(chip * CORES + cr, g)]

    def span_of(index, rows):
        return pl.ds(pl.multiple_of(index * g + rows[0], m), rows[1] - rows[0])

    def block(c, rows, chip):
        return gall.at[c, span_of(chip * CORES + core, rows)]

    def to_near(c, rows):
        b = block(c, rows, z)
        return rdma(b, b, zs.at[0], zr_near.at[c], near * CORES + core, t)

    def to_across(c, rows):
        b = block(c, rows, z)
        return rdma(b, b, zs.at[1], zr_rest.at[0 if rows == A else 1, c], across * CORES + core, t)

    def near_in(c):
        b = replica(c, near, core)
        rdma(b, b, zs.at[0], zr_near.at[c], near * CORES + core, t).wait_recv()

    def rest_in(c, rows):
        b = gall.at[c, 0:2 * (rows[1] - rows[0])]
        rdma(b, b, zs.at[0], zr_rest.at[0 if rows == A else 1, c], near * CORES + core, t).wait_recv()

    def forward(c, rows):
        for chip in (across, far):
            b = block(c, rows, chip)
            rdma(b, b, fs.at[0], zr_rest.at[0 if rows == A else 1, c], near * CORES + core, t).start()

    def mate_copy(c, chip):
        b = replica(c, chip, core)
        if chip is near:
            return rdma(b, b, ms.at[1], mr_near.at[c], mate, t)
        return rdma(b, b, ms.at[0 if chip is z else 1], mr_rest.at[c], mate, t)

    def mate_near_in(c):
        b = gall.at[c, 0:g]
        rdma(b, b, ms.at[0], mr_near.at[c], mate, t).wait_recv()

    def mate_rest_in(c, replicas):
        b = gall.at[c, 0:replicas * g]
        rdma(b, b, ms.at[0], mr_rest.at[c], mate, t).wait_recv()

    def part_copy(j):
        return rdma(part_s.at[j], part_r.at[j], rs.at[0], rr.at[j], served, t)

    def grads(c, rows):
        here = slice(*rows)
        cols = rows_of(c, hc)
        gate_pre = jnp.dot(tg[here], wv[c], preferred_element_type=F32)
        ug, gg = activation_grads(gate_pre, cotv[here, cols], upv[here, cols])
        gall[c, span_of(d, rows), :] = gg
        for k in range(rows[0] // m, rows[1] // m):
            low = k * m - rows[0]
            up_grad[rows_of(flip(t, k), m), cols] = ug[low:low + m]

    def send_near(c, rows):
        @pl.when(jnp.logical_or(outer == 1, c < ng))
        def _():
            to_near(c, rows).start()

    def send_first(c):
        to_across(c, A).start()
        send_near(c, A)

    def send_rest(c, near_rows=B):
        send_near(c, near_rows)
        to_across(c, B).start()
        mate_copy(c, z).start()

    span = dw // nc

    def term_part(n):
        rows = rows_of(n, span)
        own = rows_of(d, g)
        total = jnp.zeros((g, span), F32)
        for c in range(nc):
            total += lax.dot_general(
                gall[c, own, :], wv[c, rows, :], (((1,), (1,)), ((), ())), preferred_element_type=F32)
        term[:, rows] = total.astype(BF16)

    def step(c, grad):
        cols = rows_of(c, hc)
        first, second, change = adam(grad * scale, m1v[:, cols], m2v[:, cols])
        nm1[:, cols] = first.astype(BF16)
        nm2[:, cols] = second.astype(BF16)
        upd[:, cols] = change

    def update(c, reduced=False):
        mate_near_in(c)
        if not reduced:
            mate_rest_in(c, 3)
        step(c, jnp.dot(xt[...], gall[c], preferred_element_type=F32))

    def reduce(c, j):
        mate_rest_in(c, 3)
        rows = pl.ds(pl.multiple_of(first_rep * g, g), others * g)
        part_s[j] = jnp.dot(xtp[...], gall[c, rows, :], preferred_element_type=F32).astype(BF16)
        part_copy(j).start()

    def finish(c, j):
        mate_rest_in(c, 1)
        own = rows_of(z, CORES * g)
        grad = jnp.dot(xt[:, own], gall[c, own, :], preferred_element_type=F32)
        part_copy(j).wait_recv()
        step(c, grad + part_r[j].astype(F32))

    depth = min(W_DEPTH, nc)

    load_tok.start()
    for copy in cu_loads(0):
        copy.start()
    w_load(0).start()
    barrier = pltpu.get_barrier_semaphore()
    even = lax.rem(z, 2) == 0
    NEAR, ACROSS, PEERS, MATE = range(4)

    def tell(sem, chip):
        for cr in range(CORES):
            pl.semaphore_signal(sem, inc=1, device_id=(chip * CORES + cr, t), device_id_type=MESH)

    @pl.when(even)
    def _():
        tell(barrier, near)

    @pl.when(half == 0)
    def _():
        tell(barrier, across)

        @inner_only
        def _():
            tell(barrier, far)

    @pl.when(core == 0)
    def _():
        pl.semaphore_signal(barrier, inc=1, device_id=(mate, t), device_id_type=MESH)
    for k in range(1, nt):
        @pl.when(flip(t, k) > t)
        def _():
            pl.semaphore_signal(barrier, inc=1, device_id=(d, flip(t, k)), device_id_type=MESH)

    @phase
    def tok_load():
        load_tok.wait()

    for c in range(1, depth):
        w_load(c).start()

    @phase
    def meet():
        earlier = CORES * (z - half * lax.rem(z, 2)) + t + core

        @pl.when(earlier > 0)
        def _():
            pl.semaphore_wait(barrier, earlier)

    @pl.when(jnp.logical_not(even))
    def _():
        tell(go.at[NEAR], near)

    @pl.when(half == 1)
    def _():
        @inner_only
        def _():
            tell(go.at[ACROSS], across)
            tell(go.at[ACROSS], far)

    @pl.when(core == 1)
    def _():
        pl.semaphore_signal(go.at[MATE], inc=1, device_id=(mate, t), device_id_type=MESH)
    for k in range(1, nt):
        @pl.when(flip(t, k) < t)
        def _():
            pl.semaphore_signal(go.at[PEERS], inc=1, device_id=(d, flip(t, k)), device_id_type=MESH)
            tok_copy(k).start()

    def send_down(c):
        @pl.when(half == 1)
        def _():
            to_across(c, A).start()

        @pl.when(jnp.logical_not(even))
        def _():
            send_near(c, A)

    def send_up(c):
        @pl.when(half == 0)
        def _():
            to_across(c, A).start()

        @pl.when(even)
        def _():
            send_near(c, A)

    def own_chunk(c):
        w_load(c).wait()

        @pl.when(c + depth < nc)
        def _():
            w_load(c + depth).start()

        @pl.when(c == nc // 2)
        def _():
            for k in range(1, nt):
                for copy in cu_loads(k):
                    copy.start()
        grads(c, A)

    @phase
    def own_loads():
        cu_wait(True)

    alone = min(ALONE, ng)

    @phase
    def own_first():
        @pl.loop(0, alone)
        def _(c):
            own_chunk(c)

            @pl.when(c > 0)
            def _():
                send_down(c - 1)

    @phase
    def go_wait():
        @pl.when(t < nt - 1)
        def _():
            pl.semaphore_wait(go.at[PEERS], nt - 1 - t)
        for k in range(1, nt):
            @pl.when(flip(t, k) > t)
            def _():
                tok_copy(k).start()
        send_down(alone - 1)

        @pl.when(even)
        def _():
            pl.semaphore_wait(go.at[NEAR], CORES)

        @pl.when(half == 0)
        def _():
            pl.semaphore_wait(go.at[ACROSS], CORES)

        @pl.when(core == 0)
        def _():
            pl.semaphore_wait(go.at[MATE], 1)

        @pl.loop(0, alone)
        def _(c):
            send_up(c)

    @phase
    def own_grads():
        @pl.loop(alone, nc)
        def _(c):
            own_chunk(c)

            @pl.when(jnp.logical_and(c > alone, c <= ng))
            def _():
                send_first(c - 1)

    load_x.start()
    inner_only(load_xp.start)
    load_m1.start()
    load_m2.start()
    for cr in range(CORES):
        xp_across(cr).start()
    for cr in range(CORES):
        x_across(cr).start()
        x_near(cr).start()
    x_mate.start()
    inner_only(xp_mate.start)

    @pl.loop(ng, nc)
    def _(c):
        send_first(c)

    @phase
    def inner_forwards():
        @inner_only
        def _():
            @pl.loop(0, EARLY_LAG)
            def _(c):
                rest_in(c, A)
                forward(c, A)

            @phase
            def early_wait():
                cu_wait(False)
                tok_early.wait_recv()

            @pl.loop(0, ns)
            def _(c):
                grads(c, B_EARLY)
                rest_in(EARLY_LAG + c, A)
                forward(EARLY_LAG + c, A)
                to_near(c, B_EARLY).start()

            @pl.loop(EARLY_LAG + ns, ng)
            def _(c):
                rest_in(c, A)
                forward(c, A)

        @outer_only
        def _():
            cu_wait(False)
            tok_early.wait_recv()

    @phase
    def tok_wait():
        tok_late.wait_recv()

    @phase
    def other_grads():
        @inner_only
        def _():
            @pl.loop(0, ns)
            def _(c):
                grads(c, B_LATE)

                @pl.when(c > 0)
                def _():
                    send_rest(c - 1, B_LATE)
            grads(ns, B)
            send_rest(ns - 1, B_LATE)

        @outer_only
        def _():
            @pl.loop(0, ns + 1)
            def _(c):
                grads(c, B)

                @pl.when(c > 0)
                def _():
                    send_rest(c - 1)

        @pl.loop(ns + 1, nc)
        def _(c):
            grads(c, B)
            send_rest(c - 1)

    @phase
    def x_exchange():
        term_part(0)
        send_rest(nc - 1)
        load_x.wait()

        @inner_only
        def _():
            xp_beyond.wait_recv()
            x_forward.start()
            load_xp.wait()
            xp_mate.wait_recv()
            x_all.wait_recv()
            for k in range(1, nt):
                x2_copy(k).start()
            for k in range(1, nt):
                xp2_copy(k).start()

    @phase
    def terms():
        @pl.loop(1, nc)
        def _(n):
            term_part(n)

    @phase
    def outer_x():
        @outer_only
        def _():
            x_all.wait_recv()
            for k in range(1, nt):
                x2_copy(k).start()
            for k in range(1, nt):
                term_copy(k).start()

    def takes(c):
        @phase
        def others_in():
            near_in(c)
            mate_copy(c, near).start()

            @outer_only
            def _():
                rest_in(c, A)
            rest_in(c, B)

            @inner_only
            def _():
                forward(c, B)
            mate_copy(c, across).start()
            mate_copy(c, far).start()

    @pl.loop(0, lead)
    def _(c):
        takes(c)

    @inner_only
    def _():
        for k in range(1, nt):
            term_copy(k).start()

    @phase
    def x_wait():
        x2_all.wait_recv()

    load_m1.wait()
    load_m2.wait()

    @phase
    def transposes():
        for i in range(ndp):
            xt[:, i * g:(i + 1) * g] = xg[:, i].reshape(g, rw).T

    @pl.loop(lead, ng)
    def _(c):
        takes(c)

        @phase
        def updates():
            update(c - lead)

    def input_grads():
        with jax.named_scope("input_grads"):
            total = term[0:m, :].astype(F32)
            term_in.wait_recv()
            for k in range(1, nt):
                total += termr[k].astype(F32)
            in_grad[...] = total.astype(BF16)

    @inner_only
    def _():
        @phase
        def xp_wait():
            xp2_all.wait_recv()
            for i in range(others):
                xtp[:, i * g:(i + 1) * g] = xp[:, i].reshape(g, rw).T

        for j in range(nr):
            @phase
            def last_in():
                rest_in(ng + j, A)
                rest_in(ng + j, B)
                mate_copy(ng + j, across).start()
                mate_copy(ng + j, far).start()

            @phase
            def updates():
                update(ng - lead + j)

            @phase
            def reduces():
                reduce(ng + j, j)

            @phase
            def near_last():
                near_in(ng + j)
                mate_copy(ng + j, near).start()

        @pl.loop(ng - lead + nr, ng)
        def _(c):
            update(c)

        @pl.loop(ng, nc)
        def _(c):
            update(c, True)
        input_grads()

    @outer_only
    def _():
        @pl.loop(ng - lead, ng)
        def _(c):
            @phase
            def updates():
                update(c)
        input_grads()
        for j in range(nr):
            @phase
            def finishes():
                finish(ng + j, j)

    def sent(sem, chunks, replicas):
        b = gall.at[0:chunks, 0:replicas * g]
        rdma(b, b, sem, sem, mate, t).wait_send()

    @phase
    def drain():
        tok_all.wait_send()
        x2_all.wait_send()
        term_out.wait_send()
        x_all.wait_send()
        sent(zs.at[1], nc, 1)
        sent(ms.at[0], nc, 1)

        @outer_only
        def _():
            sent(zs.at[0], nc, 1)
            sent(ms.at[1], ng, 3)

        @inner_only
        def _():
            sent(zs.at[0], ng, 1)
            sent(ms.at[1], nc, 3)
            sent(fs.at[0], ng, 2)
            xp_mate.wait_send()
            x_forward.wait_send()
            xp2_all.wait_send()
            rdma(part_s, part_s, rs.at[0], rs.at[0], mate, t).wait_send()


def fused(ndp, nt, tokens, gate_weight, up_act, cotangent, moment1, moment2):
    m, dw = tokens.shape
    g, hid = up_act.shape
    rw = moment1.shape[0]
    nc = hid // WIDE
    nr = SUMMED * nc // 8
    any_spec, vmem = pl.BlockSpec(memory_space=pltpu.HBM), pl.BlockSpec(memory_space=pltpu.VMEM)
    dma = pltpu.SemaphoreType.DMA
    results = (((m, dw), BF16), ((g, hid), BF16), ((rw, hid), BF16), ((rw, hid), BF16), ((rw, hid), F32))
    held = pl.pallas_call(
        functools.partial(kernel, ndp, nt),
        out_shape=tuple(pltpu.VMEM(shape, dtype) for shape, dtype in results),
        in_specs=[any_spec] * 6,
        out_specs=(vmem,) * 5,
        scratch_shapes=[
            pltpu.VMEM((g, dw), BF16),
            pltpu.VMEM((nt, ndp, m, rw), BF16),
            pltpu.VMEM((nt, ndp - CORES, m, rw), BF16),
            pltpu.VMEM((rw, ndp * g), BF16),
            pltpu.VMEM((rw, (ndp - CORES) * g), BF16),
            pltpu.VMEM((nc, dw, WIDE), BF16),
            pltpu.VMEM((g, hid), BF16),
            pltpu.VMEM((g, hid), BF16),
            pltpu.VMEM((rw, hid), BF16),
            pltpu.VMEM((rw, hid), BF16),
            pltpu.VMEM((nc, ndp * g, WIDE), BF16),
            pltpu.VMEM((g, dw), BF16),
            pltpu.VMEM((nt, m, dw), BF16),
            pltpu.VMEM((nr, rw, WIDE), BF16),
            pltpu.VMEM((nr, rw, WIDE), BF16),
            dma((5,)), dma((nc,)), dma((3,)), dma((3,)), dma((6,)), dma((4,)),
            dma((2,)), dma((1,)), dma((2,)), dma((nc,)), dma((2, nc)),
            dma((nc,)), dma((nc,)), dma((1,)), dma((nr,)), dma((2,)), pltpu.SemaphoreType.REGULAR((4,)),
        ],
        compiler_params=pltpu.CompilerParams(
            collective_id=0, has_side_effects=True, vmem_limit_bytes=VMEM_BUDGET),
    )(*(pltpu.with_memory_space_constraint(x, pltpu.HBM)
        for x in (tokens, gate_weight, up_act, cotangent, moment1, moment2)))
    return pl.pallas_call(
        write_out,
        out_shape=tuple(pltpu.HBM(shape, dtype) for shape, dtype in results),
        in_specs=[vmem] * 5,
        out_specs=(any_spec,) * 5,
        scratch_shapes=[dma((5,))],
        compiler_params=pltpu.CompilerParams(vmem_limit_bytes=2**20),
    )(*(pltpu.with_memory_space_constraint(x, pltpu.VMEM) for x in held))


def write_out(*refs):
    sems = refs[-1]
    copies = [pltpu.make_async_copy(refs[i], refs[5 + i], sems.at[i]) for i in range(5)]
    for copy in reversed(copies):
        copy.start()
    for copy in copies:
        copy.wait()


def plain(ndp, nt, tokens, gate_weight, up_act, cotangent, moment1, moment2):
    gathered = lax.all_gather(tokens, "tensor", axis=0, tiled=True)
    gate_pre = jnp.dot(gathered, gate_weight, preferred_element_type=F32)
    up_grad, gate_grad = activation_grads(gate_pre, cotangent, up_act)
    term = lax.dot_general(
        gate_grad, gate_weight, (((1,), (1,)), ((), ())), preferred_element_type=F32).astype(BF16)
    in_grad = lax.psum_scatter(term, "tensor", scatter_dimension=0, tiled=True)
    partial_value = lax.dot_general(
        gathered, gate_grad, (((0,), (0,)), ((), ())), preferred_element_type=F32).astype(BF16)
    shard = lax.psum_scatter(partial_value.astype(F32), "dp", scatter_dimension=0, tiled=True)
    first, second, update = adam(shard * (1.0 / math.sqrt(ndp * gathered.shape[0])), moment1, moment2)
    return in_grad, up_grad, first.astype(BF16), second.astype(BF16), update


def local(ndp, nt, *args):
    (m, dw), (g, hid), rw = args[0].shape, args[2].shape, args[4].shape[0]
    need = (2 * dw * hid + 2 * ndp * g * (hid + 2 * rw) + 12 * g * hid + 16 * rw * hid + 16 * g * dw)
    fits = (need <= VMEM_BUDGET and hid >= 8 * WIDE and ndp == CORES * CHIPS and nt > 1 and nt & (nt - 1) == 0
            and hid % WIDE == 0 and g % 128 == 0 and rw % 128 == 0 and m % 16 == 0
            and dw % (128 * (hid // WIDE)) == 0)
    return (fused if fits else plain)(ndp, nt, *args)


def solution(mesh):
    both = P("dp", "tensor")
    rows = P(("dp", "tensor"), None)
    return jax.shard_map(
        functools.partial(local, mesh.shape["dp"], mesh.shape["tensor"]),
        mesh=mesh,
        in_specs=(rows, P(None, "tensor"), both, both, both, both),
        out_specs=(rows, both, both, both, both),
        check_vma=False,
    )
```

```python
import functools
import math

import jax
import jax.numpy as jnp
from jax import lax
from jax.experimental import pallas as pl
from jax.experimental.pallas import tpu as pltpu
from jax.sharding import PartitionSpec as P

MESH = pl.DeviceIdType.MESH
F32, BF16 = jnp.float32, jnp.bfloat16
CORES = 2
CHIPS = 4
WIDE = 256
SUMMED = 2
LEAD = 4
W_DEPTH = 3
ALONE = 2
EARLY = 3
EARLY_LAG = 2
VMEM_BUDGET = 48 * 2**20


def adam(grad, moment1, moment2):
    first = 0.9 * moment1.astype(F32) + 0.1 * grad
    second = 0.95 * moment2.astype(F32) + 0.05 * grad * grad
    return first, second, first / (jnp.sqrt(second) + 1e-08)


def activation_grads(gate_pre, cot, up):
    sig = jax.nn.sigmoid(gate_pre)
    cot = cot.astype(F32)
    up_grad = (cot * gate_pre * sig).astype(BF16)
    gate_grad = (cot * up.astype(F32) * sig * (1.0 + gate_pre * (1.0 - sig))).astype(BF16)
    return up_grad, gate_grad


def phase(run):
    with jax.named_scope(run.__name__):
        run()


def flip(t, k):
    bit = 1
    while bit <= k:
        if k & bit:
            t = t + bit - 2 * bit * lax.rem(t // bit, 2)
        bit *= 2
    return t


def kernel(ndp, nt, tok, w, up, cot, m1, m2, in_grad, up_grad, nm1, nm2, upd,
           tg, xg, xp, xt, xtp, wv, upv, cotv, m1v, m2v, gall, term, termr, part_s, part_r,
           loc_sem, w_sem, cu_sem, tok_sem, x_sem, x2_sem, zs, fs, ms, zr_near, zr_rest,
           mr, rs, rr, term_sem, go):
    d, t = lax.axis_index("dp"), lax.axis_index("tensor")
    z, core = d // CORES, lax.rem(d, CORES)
    mate = d + 1 - 2 * core
    m, dw = tok.shape
    g, hid = up.shape
    rw = m1.shape[0]
    nc, _, hc = wv.shape
    nr = part_s.shape[0]
    ng = nc - nr
    lead = min(LEAD, ng)
    early = (nt // 2 + 1) * m
    A, B, B_EARLY, B_LATE = (0, m), (m, g), (m, early), (early, g)
    ns = min(EARLY, ng - EARLY_LAG)
    scale = 1.0 / math.sqrt(ndp * g)

    half = z // 2
    near = z + 1 - 2 * lax.rem(z, 2)
    across = 2 - half
    far = 3 - 3 * half
    outer = lax.rem(z + half + 1, 2)
    first_rep = CORES * (1 - half)
    others = ndp - CORES
    beyond = others - CORES

    def inner_only(run):
        pl.when(outer == 0)(run)

    def outer_only(run):
        pl.when(outer == 1)(run)

    def rdma(src, dst, s, r, dp, tn):
        return pltpu.make_async_remote_copy(
            src_ref=src, dst_ref=dst, send_sem=s, recv_sem=r, device_id=(dp, tn), device_id_type=MESH)

    def rows_of(i, size):
        return pl.ds(pl.multiple_of(i * size, size), size)

    served = near * CORES + 1 - core

    load_tok = pltpu.make_async_copy(tok, tg.at[0:m], loc_sem.at[0])
    load_x = pltpu.make_async_copy(tok.at[:, rows_of(d, rw)], xg.at[0, d], loc_sem.at[1])
    load_xp = pltpu.make_async_copy(tok.at[:, rows_of(served, rw)], xp.at[0, d - first_rep], loc_sem.at[4])
    load_m1 = pltpu.make_async_copy(m1, m1v, loc_sem.at[2])
    load_m2 = pltpu.make_async_copy(m2, m2v, loc_sem.at[3])

    def w_load(c):
        return pltpu.make_async_copy(w.at[:, rows_of(c, hc)], wv.at[c], w_sem.at[lax.rem(c, W_DEPTH)])

    def cu_loads(k):
        src = rows_of(flip(t, k), m)
        dst = pl.ds(k * m, m)
        return (pltpu.make_async_copy(cot.at[src], cotv.at[dst], cu_sem.at[1 if k else 0]),
                pltpu.make_async_copy(up.at[src], upv.at[dst], cu_sem.at[2 if k else 0]))

    def cu_wait(first):
        if first:
            pltpu.make_async_copy(cot.at[0:2 * m], cotv.at[0:2 * m], cu_sem.at[0]).wait()
        else:
            pltpu.make_async_copy(cot.at[m:g], cotv.at[m:g], cu_sem.at[1]).wait()
            pltpu.make_async_copy(up.at[m:g], upv.at[m:g], cu_sem.at[2]).wait()

    def tok_copy(k):
        return rdma(tg.at[0:m], tg.at[k * m:(k + 1) * m], tok_sem.at[0],
                    tok_sem.at[1 if k * m < early else 2], d, flip(t, k))

    tok_all = rdma(tg.at[m:g], tg.at[m:g], tok_sem.at[0], tok_sem.at[1], mate, t)
    tok_early = rdma(tg.at[m:early], tg.at[m:early], tok_sem.at[0], tok_sem.at[1], mate, t)
    tok_late = rdma(tg.at[early:g], tg.at[early:g], tok_sem.at[0], tok_sem.at[2], mate, t)

    def features(chip, cr):
        return tg.at[0:m, rows_of(chip * CORES + cr, rw)]

    def x_near(cr):
        return rdma(features(near, cr), xg.at[0, d], x_sem.at[0], x_sem.at[1], near * CORES + cr, t)

    def x_across(cr):
        return rdma(features(across, cr), xg.at[0, d], x_sem.at[0], x_sem.at[1], across * CORES + cr, t)

    def xp_across(cr):
        return rdma(features(far, 1 - cr), xp.at[0, d - CORES * half], x_sem.at[0], x_sem.at[2],
                    across * CORES + cr, t)

    x_mate = rdma(features(z, 1 - core), xg.at[0, d], x_sem.at[0], x_sem.at[1], mate, t)
    xp_mate = rdma(features(near, core), xp.at[0, d - first_rep], x_sem.at[3], x_sem.at[4], mate, t)
    x_forward = rdma(xp.at[0, pl.ds(first_rep, beyond)], xg.at[0, pl.ds(CORES * first_rep, beyond)],
                     x_sem.at[5], x_sem.at[1], served, t)
    x_all = rdma(xg.at[0, 0:ndp - 1], xg.at[0, 0:ndp - 1], x_sem.at[0], x_sem.at[1], mate, t)
    xp_beyond = rdma(xp.at[0, 0:beyond], xp.at[0, 0:beyond], x_sem.at[5], x_sem.at[2], mate, t)

    def x2_copy(k):
        return rdma(xg.at[0], xg.at[k], x2_sem.at[0], x2_sem.at[1], d, flip(t, k))

    def xp2_copy(k):
        return rdma(xp.at[0], xp.at[k], x2_sem.at[2], x2_sem.at[3], d, flip(t, k))

    x2_all = rdma(xg.at[1:nt], xg.at[1:nt], x2_sem.at[0], x2_sem.at[1], mate, t)
    xp2_all = rdma(xp.at[1:nt], xp.at[1:nt], x2_sem.at[2], x2_sem.at[3], mate, t)

    def term_copy(k):
        return rdma(term.at[k * m:(k + 1) * m], termr.at[k], term_sem.at[0], term_sem.at[1], d, flip(t, k))

    term_out = rdma(term.at[m:g], term.at[m:g], term_sem.at[0], term_sem.at[1], mate, t)
    term_in = rdma(termr.at[1:nt], termr.at[1:nt], term_sem.at[0], term_sem.at[1], mate, t)

    def replica(c, chip, cr):
        return gall.at[c, rows_of(chip * CORES + cr, g)]

    def span_of(index, rows):
        return pl.ds(pl.multiple_of(index * g + rows[0], m), rows[1] - rows[0])

    def block(c, rows, chip):
        return gall.at[c, span_of(chip * CORES + core, rows)]

    def to_near(c, rows):
        b = block(c, rows, z)
        return rdma(b, b, zs.at[0], zr_near.at[c], near * CORES + core, t)

    def to_across(c, rows):
        b = block(c, rows, z)
        return rdma(b, b, zs.at[1], zr_rest.at[0 if rows == A else 1, c], across * CORES + core, t)

    def near_in(c):
        b = replica(c, near, core)
        rdma(b, b, zs.at[0], zr_near.at[c], near * CORES + core, t).wait_recv()

    def rest_in(c, rows):
        b = gall.at[c, 0:2 * (rows[1] - rows[0])]
        rdma(b, b, zs.at[0], zr_rest.at[0 if rows == A else 1, c], near * CORES + core, t).wait_recv()

    def forward(c, rows):
        for chip in (across, far):
            b = block(c, rows, chip)
            rdma(b, b, fs.at[0], zr_rest.at[0 if rows == A else 1, c], near * CORES + core, t).start()

    def mate_copy(c, chip):
        b = replica(c, chip, core)
        return rdma(b, b, ms.at[0 if chip is z else 1], mr.at[c], mate, t)

    def mate_last(j):
        b = replica(ng + j, near, core)
        return rdma(b, b, ms.at[1], mr.at[nc + j], mate, t)

    def mate_in(c, replicas):
        b = gall.at[0, 0:replicas * g]
        rdma(b, b, ms.at[0], mr.at[c], mate, t).wait_recv()

    def part_copy(j):
        return rdma(part_s.at[j], part_r.at[j], rs.at[0], rr.at[j], served, t)

    def grads(c, rows):
        here = slice(*rows)
        cols = rows_of(c, hc)
        gate_pre = jnp.dot(tg[here], wv[c], preferred_element_type=F32)
        ug, gg = activation_grads(gate_pre, cotv[here, cols], upv[here, cols])
        gall[c, span_of(d, rows), :] = gg
        for k in range(rows[0] // m, rows[1] // m):
            low = k * m - rows[0]
            up_grad[rows_of(flip(t, k), m), cols] = ug[low:low + m]

    def send_near(c, rows):
        @pl.when(jnp.logical_or(outer == 1, c < ng))
        def _():
            to_near(c, rows).start()

    def send_first(c):
        to_across(c, A).start()
        send_near(c, A)

    def send_rest(c, near_rows=B):
        send_near(c, near_rows)
        to_across(c, B).start()
        mate_copy(c, z).start()

    span = dw // nc

    def term_part(n):
        rows = rows_of(n, span)
        own = rows_of(d, g)
        total = jnp.zeros((g, span), F32)
        for c in range(nc):
            total += lax.dot_general(
                gall[c, own, :], wv[c, rows, :], (((1,), (1,)), ((), ())), preferred_element_type=F32)
        term[:, rows] = total.astype(BF16)

    def step(c, grad):
        cols = rows_of(c, hc)
        first, second, change = adam(grad * scale, m1v[:, cols], m2v[:, cols])
        nm1[:, cols] = first.astype(BF16)
        nm2[:, cols] = second.astype(BF16)
        upd[:, cols] = change

    def update(c, reduced=False):
        if reduced:
            mate_in(c + nr, 1)
        else:
            mate_in(c, 4)
        step(c, jnp.dot(xt[...], gall[c], preferred_element_type=F32))

    def reduce(c, j):
        mate_in(c, 3)
        rows = pl.ds(pl.multiple_of(first_rep * g, g), others * g)
        part_s[j] = jnp.dot(xtp[...], gall[c, rows, :], preferred_element_type=F32).astype(BF16)
        part_copy(j).start()

    def finish(c, j):
        mate_in(c, 1)
        own = rows_of(z, CORES * g)
        grad = jnp.dot(xt[:, own], gall[c, own, :], preferred_element_type=F32)
        part_copy(j).wait_recv()
        step(c, grad + part_r[j].astype(F32))

    depth = W_DEPTH

    load_tok.start()
    for copy in cu_loads(0):
        copy.start()
    w_load(0).start()
    barrier = pltpu.get_barrier_semaphore()
    even = lax.rem(z, 2) == 0
    NEAR, ACROSS, MATE = range(3)

    def tell(sem, chip):
        for cr in range(CORES):
            pl.semaphore_signal(sem, inc=1, device_id=(chip * CORES + cr, t), device_id_type=MESH)

    @pl.when(even)
    def _():
        tell(barrier, near)

    @pl.when(half == 0)
    def _():
        tell(barrier, across)

        @inner_only
        def _():
            tell(barrier, far)

    @pl.when(core == 0)
    def _():
        pl.semaphore_signal(barrier, inc=1, device_id=(mate, t), device_id_type=MESH)
    for k in range(1, nt):
        @pl.when(flip(t, k) > t)
        def _():
            pl.semaphore_signal(barrier, inc=1, device_id=(d, flip(t, k)), device_id_type=MESH)

    @phase
    def meet():
        earlier = CORES * (z - half * lax.rem(z, 2)) + t + core

        @pl.when(earlier > 0)
        def _():
            pl.semaphore_wait(barrier, earlier)

    @pl.when(jnp.logical_not(even))
    def _():
        tell(go.at[NEAR], near)

    @pl.when(half == 1)
    def _():
        @inner_only
        def _():
            tell(go.at[ACROSS], across)
            tell(go.at[ACROSS], far)

    @pl.when(core == 1)
    def _():
        pl.semaphore_signal(go.at[MATE], inc=1, device_id=(mate, t), device_id_type=MESH)
    for k in range(1, nt):
        @pl.when(flip(t, k) < t)
        def _():
            pl.semaphore_signal(go.at[MATE + k], inc=1, device_id=(d, flip(t, k)), device_id_type=MESH)

    @phase
    def tok_load():
        load_tok.wait()

    for c in range(1, depth):
        w_load(c).start()

    for k in range(1, nt):
        pl.when(flip(t, k) < t)(tok_copy(k).start)

    def send_down(c):
        @pl.when(half == 1)
        def _():
            to_across(c, A).start()

        @pl.when(jnp.logical_not(even))
        def _():
            send_near(c, A)

    def send_up(c):
        @pl.when(half == 0)
        def _():
            to_across(c, A).start()

        @pl.when(even)
        def _():
            send_near(c, A)

    def own_chunk(c):
        w_load(c).wait()

        @pl.when(c + depth < nc)
        def _():
            w_load(c + depth).start()

        @pl.when(c == nc // 2)
        def _():
            for k in range(1, nt):
                for copy in cu_loads(k):
                    copy.start()
        grads(c, A)

    @phase
    def own_loads():
        cu_wait(True)

    alone = min(ALONE, ng)

    @phase
    def own_first():
        @pl.loop(0, alone)
        def _(c):
            own_chunk(c)

            @pl.when(c > 0)
            def _():
                send_down(c - 1)

    @phase
    def go_wait():
        for k in range(1, nt):
            @pl.when(flip(t, k) > t)
            def _():
                pl.semaphore_wait(go.at[MATE + k], 1)
                tok_copy(k).start()
        send_down(alone - 1)

        @pl.when(even)
        def _():
            pl.semaphore_wait(go.at[NEAR], CORES)

        @pl.when(half == 0)
        def _():
            pl.semaphore_wait(go.at[ACROSS], CORES)

        @pl.when(core == 0)
        def _():
            pl.semaphore_wait(go.at[MATE], 1)

        @pl.loop(0, alone)
        def _(c):
            send_up(c)

    @phase
    def own_grads():
        @pl.loop(alone, nc)
        def _(c):
            own_chunk(c)

            @pl.when(jnp.logical_and(c > alone, c <= ng))
            def _():
                send_first(c - 1)

    load_x.start()
    inner_only(load_xp.start)
    load_m1.start()
    load_m2.start()
    for cr in range(CORES):
        xp_across(cr).start()
    for cr in range(CORES):
        x_across(cr).start()
        x_near(cr).start()
    x_mate.start()
    inner_only(xp_mate.start)

    @pl.loop(ng, nc)
    def _(c):
        send_first(c)

    @phase
    def inner_forwards():
        @inner_only
        def _():
            @pl.loop(0, EARLY_LAG)
            def _(c):
                rest_in(c, A)
                forward(c, A)

            @phase
            def early_wait():
                cu_wait(False)
                tok_early.wait_recv()

            @pl.loop(0, ns)
            def _(c):
                grads(c, B_EARLY)
                rest_in(EARLY_LAG + c, A)
                forward(EARLY_LAG + c, A)
                to_near(c, B_EARLY).start()

            @pl.loop(EARLY_LAG + ns, ng)
            def _(c):
                rest_in(c, A)
                forward(c, A)

        @outer_only
        def _():
            cu_wait(False)
            tok_early.wait_recv()

    @phase
    def tok_wait():
        tok_late.wait_recv()

    @phase
    def other_grads():
        @inner_only
        def _():
            @pl.loop(0, ns)
            def _(c):
                grads(c, B_LATE)

                @pl.when(c > 0)
                def _():
                    send_rest(c - 1, B_LATE)
            grads(ns, B)
            send_rest(ns - 1, B_LATE)

        @outer_only
        def _():
            @pl.loop(0, ns + 1)
            def _(c):
                grads(c, B)

                @pl.when(c > 0)
                def _():
                    send_rest(c - 1)

        @pl.loop(ns + 1, nc)
        def _(c):
            grads(c, B)
            send_rest(c - 1)

    @phase
    def x_exchange():
        term_part(0)
        send_rest(nc - 1)
        load_x.wait()

        @inner_only
        def _():
            xp_beyond.wait_recv()
            x_forward.start()
            load_xp.wait()
            xp_mate.wait_recv()
            x_all.wait_recv()
            for k in range(1, nt):
                x2_copy(k).start()
            for k in range(1, nt):
                xp2_copy(k).start()

    @phase
    def terms():
        @pl.loop(1, nc)
        def _(n):
            term_part(n)

    @phase
    def outer_x():
        @outer_only
        def _():
            x_all.wait_recv()
            for k in range(1, nt):
                x2_copy(k).start()
            for k in range(1, nt):
                term_copy(k).start()

    def takes(c):
        @phase
        def others_in():
            near_in(c)
            mate_copy(c, near).start()

            @outer_only
            def _():
                rest_in(c, A)
            rest_in(c, B)

            @inner_only
            def _():
                forward(c, B)
            mate_copy(c, across).start()
            mate_copy(c, far).start()

    @pl.loop(0, lead)
    def _(c):
        takes(c)

    @inner_only
    def _():
        for k in range(1, nt):
            term_copy(k).start()

    @phase
    def x_wait():
        x2_all.wait_recv()

    load_m1.wait()
    load_m2.wait()

    @phase
    def transposes():
        for i in range(ndp):
            xt[:, i * g:(i + 1) * g] = xg[:, i].reshape(g, rw).T

    @pl.loop(lead, ng)
    def _(c):
        takes(c)

        @phase
        def updates():
            update(c - lead)

    def input_grads():
        with jax.named_scope("input_grads"):
            total = term[0:m, :].astype(F32)
            term_in.wait_recv()
            for k in range(1, nt):
                total += termr[k].astype(F32)
            in_grad[...] = total.astype(BF16)

    @inner_only
    def _():
        @phase
        def xp_wait():
            xp2_all.wait_recv()
            for i in range(others):
                xtp[:, i * g:(i + 1) * g] = xp[:, i].reshape(g, rw).T

        for j in range(nr):
            @phase
            def last_in():
                rest_in(ng + j, A)
                rest_in(ng + j, B)
                mate_copy(ng + j, across).start()
                mate_copy(ng + j, far).start()

            @phase
            def updates():
                update(ng - lead + j)

            @phase
            def reduces():
                reduce(ng + j, j)

            @phase
            def near_last():
                near_in(ng + j)
                mate_last(j).start()

        @pl.loop(ng - lead + nr, ng)
        def _(c):
            update(c)

        @pl.loop(ng, nc)
        def _(c):
            update(c, True)
        input_grads()

    @outer_only
    def _():
        @pl.loop(ng - lead, ng)
        def _(c):
            @phase
            def updates():
                update(c)
        input_grads()
        for j in range(nr):
            @phase
            def finishes():
                finish(ng + j, j)

    def sent(sem, chunks, replicas):
        b = gall.at[0:chunks, 0:replicas * g]
        rdma(b, b, sem, sem, mate, t).wait_send()

    @phase
    def drain():
        tok_all.wait_send()
        x2_all.wait_send()
        term_out.wait_send()
        x_all.wait_send()
        sent(zs.at[1], nc, 1)
        sent(ms.at[0], nc, 1)

        @outer_only
        def _():
            sent(zs.at[0], nc, 1)
            sent(ms.at[1], ng, 3)

        @inner_only
        def _():
            sent(zs.at[0], ng, 1)
            sent(ms.at[1], nc, 3)
            sent(fs.at[0], ng, 2)
            xp_mate.wait_send()
            x_forward.wait_send()
            xp2_all.wait_send()
            rdma(part_s, part_s, rs.at[0], rs.at[0], mate, t).wait_send()


def fused(ndp, nt, tokens, gate_weight, up_act, cotangent, moment1, moment2):
    m, dw = tokens.shape
    g, hid = up_act.shape
    rw = moment1.shape[0]
    nc = hid // WIDE
    nr = SUMMED * nc // 8
    any_spec, vmem = pl.BlockSpec(memory_space=pltpu.HBM), pl.BlockSpec(memory_space=pltpu.VMEM)
    dma = pltpu.SemaphoreType.DMA
    results = (((m, dw), BF16), ((g, hid), BF16), ((rw, hid), BF16), ((rw, hid), BF16), ((rw, hid), F32))
    held = pl.pallas_call(
        functools.partial(kernel, ndp, nt),
        out_shape=tuple(pltpu.VMEM(shape, dtype) for shape, dtype in results),
        in_specs=[any_spec] * 6,
        out_specs=(vmem,) * 5,
        scratch_shapes=[
            pltpu.VMEM((g, dw), BF16),
            pltpu.VMEM((nt, ndp, m, rw), BF16),
            pltpu.VMEM((nt, ndp - CORES, m, rw), BF16),
            pltpu.VMEM((rw, ndp * g), BF16),
            pltpu.VMEM((rw, (ndp - CORES) * g), BF16),
            pltpu.VMEM((nc, dw, WIDE), BF16),
            pltpu.VMEM((g, hid), BF16),
            pltpu.VMEM((g, hid), BF16),
            pltpu.VMEM((rw, hid), BF16),
            pltpu.VMEM((rw, hid), BF16),
            pltpu.VMEM((nc, ndp * g, WIDE), BF16),
            pltpu.VMEM((g, dw), BF16),
            pltpu.VMEM((nt, m, dw), BF16),
            pltpu.VMEM((nr, rw, WIDE), BF16),
            pltpu.VMEM((nr, rw, WIDE), BF16),
            dma((5,)), dma((W_DEPTH,)), dma((3,)), dma((3,)), dma((6,)), dma((4,)),
            dma((2,)), dma((1,)), dma((2,)), dma((nc,)), dma((2, nc)),
            dma((nc + nr,)), dma((1,)), dma((nr,)), dma((2,)), pltpu.SemaphoreType.REGULAR((2 + nt,)),
        ],
        compiler_params=pltpu.CompilerParams(
            collective_id=0, has_side_effects=True, vmem_limit_bytes=VMEM_BUDGET),
    )(*(pltpu.with_memory_space_constraint(x, pltpu.HBM)
        for x in (tokens, gate_weight, up_act, cotangent, moment1, moment2)))
    return pl.pallas_call(
        write_out,
        out_shape=tuple(pltpu.HBM(shape, dtype) for shape, dtype in results),
        in_specs=[vmem] * 5,
        out_specs=(any_spec,) * 5,
        scratch_shapes=[dma((5,))],
        compiler_params=pltpu.CompilerParams(vmem_limit_bytes=2**20),
    )(*(pltpu.with_memory_space_constraint(x, pltpu.VMEM) for x in held))


def write_out(*refs):
    sems = refs[-1]
    copies = [pltpu.make_async_copy(refs[i], refs[5 + i], sems.at[i]) for i in range(5)]
    for copy in reversed(copies):
        copy.start()
    for copy in copies:
        copy.wait()


def plain(ndp, nt, tokens, gate_weight, up_act, cotangent, moment1, moment2):
    gathered = lax.all_gather(tokens, "tensor", axis=0, tiled=True)
    gate_pre = jnp.dot(gathered, gate_weight, preferred_element_type=F32)
    up_grad, gate_grad = activation_grads(gate_pre, cotangent, up_act)
    term = lax.dot_general(
        gate_grad, gate_weight, (((1,), (1,)), ((), ())), preferred_element_type=F32).astype(BF16)
    in_grad = lax.psum_scatter(term, "tensor", scatter_dimension=0, tiled=True)
    partial_value = lax.dot_general(
        gathered, gate_grad, (((0,), (0,)), ((), ())), preferred_element_type=F32).astype(BF16)
    shard = lax.psum_scatter(partial_value.astype(F32), "dp", scatter_dimension=0, tiled=True)
    first, second, update = adam(shard * (1.0 / math.sqrt(ndp * gathered.shape[0])), moment1, moment2)
    return in_grad, up_grad, first.astype(BF16), second.astype(BF16), update


def local(ndp, nt, *args):
    (m, dw), (g, hid), rw = args[0].shape, args[2].shape, args[4].shape[0]
    need = (2 * dw * hid + 2 * ndp * g * (hid + 2 * rw) + 12 * g * hid + 16 * rw * hid + 16 * g * dw)
    fits = (need <= VMEM_BUDGET and hid >= 8 * WIDE and ndp == CORES * CHIPS and nt > 1 and nt & (nt - 1) == 0
            and hid % WIDE == 0 and g % 128 == 0 and rw % 128 == 0 and m % 16 == 0
            and dw % (128 * (hid // WIDE)) == 0)
    return (fused if fits else plain)(ndp, nt, *args)


def solution(mesh):
    both = P("dp", "tensor")
    rows = P(("dp", "tensor"), None)
    return jax.shard_map(
        functools.partial(local, mesh.shape["dp"], mesh.shape["tensor"]),
        mesh=mesh,
        in_specs=(rows, P(None, "tensor"), both, both, both, both),
        out_specs=(rows, both, both, both, both),
        check_vma=False,
    )
```

```python
import functools
import math

import jax
import jax.numpy as jnp
from jax import lax
from jax.experimental import pallas as pl
from jax.experimental.pallas import tpu as pltpu
from jax.sharding import PartitionSpec as P

MESH = pl.DeviceIdType.MESH
F32, BF16 = jnp.float32, jnp.bfloat16
CORES = 2
CHIPS = 4
WIDE = 256
SUMMED = 2
LEAD = 4
W_DEPTH = 3
ALONE = 2
EARLY = 4
EARLY_LAG = 2
VMEM_BUDGET = 48 * 2**20


def adam(grad, moment1, moment2):
    first = 0.9 * moment1.astype(F32) + 0.1 * grad
    second = 0.95 * moment2.astype(F32) + 0.05 * grad * grad
    return first, second, first / (jnp.sqrt(second) + 1e-08)


def activation_grads(gate_pre, cot, up):
    sig = jax.nn.sigmoid(gate_pre)
    cot = cot.astype(F32)
    up_grad = (cot * gate_pre * sig).astype(BF16)
    gate_grad = (cot * up.astype(F32) * sig * (1.0 + gate_pre * (1.0 - sig))).astype(BF16)
    return up_grad, gate_grad


def phase(run):
    with jax.named_scope(run.__name__):
        run()


def flip(t, k):
    bit = 1
    while bit <= k:
        if k & bit:
            t = t + bit - 2 * bit * lax.rem(t // bit, 2)
        bit *= 2
    return t


def kernel(ndp, nt, tok, w, up, cot, m1, m2, in_grad, up_grad, nm1, nm2, upd,
           tg, xg, xp, xt, xtp, wv, upv, cotv, m1v, m2v, gall, term, termr, part_s, part_r,
           loc_sem, w_sem, cu_sem, tok_sem, x_sem, x2_sem, zs, fs, ms, zr_near, zr_rest,
           mr, rs, rr, term_sem, go):
    d, t = lax.axis_index("dp"), lax.axis_index("tensor")
    z, core = d // CORES, lax.rem(d, CORES)
    mate = d + 1 - 2 * core
    m, dw = tok.shape
    g, hid = up.shape
    rw = m1.shape[0]
    nc, _, hc = wv.shape
    nr = part_s.shape[0]
    ng = nc - nr
    lead = min(LEAD, ng)
    early = (nt // 2 + 1) * m
    A, B, B_EARLY, B_LATE = (0, m), (m, g), (m, early), (early, g)
    ns = min(EARLY, ng - EARLY_LAG)
    scale = 1.0 / math.sqrt(ndp * g)

    half = z // 2
    near = z + 1 - 2 * lax.rem(z, 2)
    across = 2 - half
    far = 3 - 3 * half
    outer = lax.rem(z + half + 1, 2)
    first_rep = CORES * (1 - half)
    others = ndp - CORES
    beyond = others - CORES

    def inner_only(run):
        pl.when(outer == 0)(run)

    def outer_only(run):
        pl.when(outer == 1)(run)

    def rdma(src, dst, s, r, dp, tn):
        return pltpu.make_async_remote_copy(
            src_ref=src, dst_ref=dst, send_sem=s, recv_sem=r, device_id=(dp, tn), device_id_type=MESH)

    def rows_of(i, size):
        return pl.ds(pl.multiple_of(i * size, size), size)

    served = near * CORES + 1 - core

    load_tok = pltpu.make_async_copy(tok, tg.at[0:m], loc_sem.at[0])
    load_x = pltpu.make_async_copy(tok.at[:, rows_of(d, rw)], xg.at[0, d], loc_sem.at[1])
    load_xp = pltpu.make_async_copy(tok.at[:, rows_of(served, rw)], xp.at[0, d - first_rep], loc_sem.at[4])
    load_m1 = pltpu.make_async_copy(m1, m1v, loc_sem.at[2])
    load_m2 = pltpu.make_async_copy(m2, m2v, loc_sem.at[3])

    def w_load(c):
        return pltpu.make_async_copy(w.at[:, rows_of(c, hc)], wv.at[c], w_sem.at[lax.rem(c, W_DEPTH)])

    def cu_loads(k):
        src = rows_of(flip(t, k), m)
        dst = pl.ds(k * m, m)
        return (pltpu.make_async_copy(cot.at[src], cotv.at[dst], cu_sem.at[1 if k else 0]),
                pltpu.make_async_copy(up.at[src], upv.at[dst], cu_sem.at[2 if k else 0]))

    def cu_wait(first):
        if first:
            pltpu.make_async_copy(cot.at[0:2 * m], cotv.at[0:2 * m], cu_sem.at[0]).wait()
        else:
            pltpu.make_async_copy(cot.at[m:g], cotv.at[m:g], cu_sem.at[1]).wait()
            pltpu.make_async_copy(up.at[m:g], upv.at[m:g], cu_sem.at[2]).wait()

    def tok_copy(k):
        return rdma(tg.at[0:m], tg.at[k * m:(k + 1) * m], tok_sem.at[0],
                    tok_sem.at[1 if k * m < early else 2], d, flip(t, k))

    tok_all = rdma(tg.at[m:g], tg.at[m:g], tok_sem.at[0], tok_sem.at[1], mate, t)
    tok_early = rdma(tg.at[m:early], tg.at[m:early], tok_sem.at[0], tok_sem.at[1], mate, t)
    tok_late = rdma(tg.at[early:g], tg.at[early:g], tok_sem.at[0], tok_sem.at[2], mate, t)

    def features(chip, cr):
        return tg.at[0:m, rows_of(chip * CORES + cr, rw)]

    def x_near(cr):
        return rdma(features(near, cr), xg.at[0, d], x_sem.at[0], x_sem.at[1], near * CORES + cr, t)

    def x_across(cr):
        return rdma(features(across, cr), xg.at[0, d], x_sem.at[0], x_sem.at[1], across * CORES + cr, t)

    def xp_across(cr):
        return rdma(features(far, 1 - cr), xp.at[0, d - CORES * half], x_sem.at[0], x_sem.at[2],
                    across * CORES + cr, t)

    x_mate = rdma(features(z, 1 - core), xg.at[0, d], x_sem.at[0], x_sem.at[1], mate, t)
    xp_mate = rdma(features(near, core), xp.at[0, d - first_rep], x_sem.at[3], x_sem.at[4], mate, t)
    x_forward = rdma(xp.at[0, pl.ds(first_rep, beyond)], xg.at[0, pl.ds(CORES * first_rep, beyond)],
                     x_sem.at[5], x_sem.at[1], served, t)
    x_all = rdma(xg.at[0, 0:ndp - 1], xg.at[0, 0:ndp - 1], x_sem.at[0], x_sem.at[1], mate, t)
    xp_beyond = rdma(xp.at[0, 0:beyond], xp.at[0, 0:beyond], x_sem.at[5], x_sem.at[2], mate, t)

    def x2_copy(k):
        return rdma(xg.at[0], xg.at[k], x2_sem.at[0], x2_sem.at[1], d, flip(t, k))

    def xp2_copy(k):
        return rdma(xp.at[0], xp.at[k], x2_sem.at[2], x2_sem.at[3], d, flip(t, k))

    x2_all = rdma(xg.at[1:nt], xg.at[1:nt], x2_sem.at[0], x2_sem.at[1], mate, t)
    xp2_all = rdma(xp.at[1:nt], xp.at[1:nt], x2_sem.at[2], x2_sem.at[3], mate, t)

    def term_copy(k):
        return rdma(term.at[k * m:(k + 1) * m], termr.at[k], term_sem.at[0], term_sem.at[1], d, flip(t, k))

    term_out = rdma(term.at[m:g], term.at[m:g], term_sem.at[0], term_sem.at[1], mate, t)
    term_in = rdma(termr.at[1:nt], termr.at[1:nt], term_sem.at[0], term_sem.at[1], mate, t)

    def replica(c, chip, cr):
        return gall.at[c, rows_of(chip * CORES + cr, g)]

    def span_of(index, rows):
        return pl.ds(pl.multiple_of(index * g + rows[0], m), rows[1] - rows[0])

    def block(c, rows, chip):
        return gall.at[c, span_of(chip * CORES + core, rows)]

    def to_near(c, rows):
        b = block(c, rows, z)
        return rdma(b, b, zs.at[0], zr_near.at[c], near * CORES + core, t)

    def to_across(c, rows):
        b = block(c, rows, z)
        return rdma(b, b, zs.at[1], zr_rest.at[0 if rows == A else 1, c], across * CORES + core, t)

    def near_in(c):
        b = replica(c, near, core)
        rdma(b, b, zs.at[0], zr_near.at[c], near * CORES + core, t).wait_recv()

    def rest_in(c, rows):
        b = gall.at[c, 0:2 * (rows[1] - rows[0])]
        rdma(b, b, zs.at[0], zr_rest.at[0 if rows == A else 1, c], near * CORES + core, t).wait_recv()

    def forward(c, rows):
        for chip in (across, far):
            b = block(c, rows, chip)
            rdma(b, b, fs.at[0], zr_rest.at[0 if rows == A else 1, c], near * CORES + core, t).start()

    def mate_copy(c, chip):
        b = replica(c, chip, core)
        return rdma(b, b, ms.at[0 if chip is z else 1], mr.at[c], mate, t)

    def mate_last(j):
        b = replica(ng + j, near, core)
        return rdma(b, b, ms.at[1], mr.at[nc + j], mate, t)

    def mate_in(c, replicas):
        b = gall.at[0, 0:replicas * g]
        rdma(b, b, ms.at[0], mr.at[c], mate, t).wait_recv()

    halves = [slice(0, rw // 2), slice(rw // 2, rw)]

    def part_copy(j, h):
        return rdma(part_s.at[j, halves[h]], part_r.at[j, halves[h]], rs.at[0], rr.at[j, h], served, t)

    def grads(c, rows):
        here = slice(*rows)
        cols = rows_of(c, hc)
        gate_pre = jnp.dot(tg[here], wv[c], preferred_element_type=F32)
        ug, gg = activation_grads(gate_pre, cotv[here, cols], upv[here, cols])
        gall[c, span_of(d, rows), :] = gg
        for k in range(rows[0] // m, rows[1] // m):
            low = k * m - rows[0]
            up_grad[rows_of(flip(t, k), m), cols] = ug[low:low + m]

    def send_near(c, rows):
        @pl.when(jnp.logical_or(outer == 1, c < ng))
        def _():
            to_near(c, rows).start()

    def send_first(c):
        to_across(c, A).start()
        send_near(c, A)

    def send_rest(c, near_rows=B):
        send_near(c, near_rows)
        to_across(c, B).start()
        mate_copy(c, z).start()

    span = dw // nc

    def term_part(n):
        rows = rows_of(n, span)
        own = rows_of(d, g)
        total = jnp.zeros((g, span), F32)
        for c in range(nc):
            total += lax.dot_general(
                gall[c, own, :], wv[c, rows, :], (((1,), (1,)), ((), ())), preferred_element_type=F32)
        term[:, rows] = total.astype(BF16)

    def step(c, grad, rows=slice(None)):
        cols = rows_of(c, hc)
        first, second, change = adam(grad * scale, m1v[rows, cols], m2v[rows, cols])
        nm1[rows, cols] = first.astype(BF16)
        nm2[rows, cols] = second.astype(BF16)
        upd[rows, cols] = change

    def update(c, reduced=False):
        if reduced:
            mate_in(c + nr, 1)
        else:
            mate_in(c, 4)
        step(c, jnp.dot(xt[...], gall[c], preferred_element_type=F32))

    def reduce(c, j):
        mate_in(c, 3)
        rows = pl.ds(pl.multiple_of(first_rep * g, g), others * g)
        for h, part in enumerate(halves):
            part_s[j, part, :] = jnp.dot(
                xtp[part, :], gall[c, rows, :], preferred_element_type=F32).astype(BF16)
            part_copy(j, h).start()

    def finish(c, j):
        mate_in(c, 1)
        own = rows_of(z, CORES * g)
        grad = jnp.dot(xt[:, own], gall[c, own, :], preferred_element_type=F32)
        for h, part in enumerate(halves):
            part_copy(j, h).wait_recv()
            step(c, grad[part] + part_r[j, part, :].astype(F32), part)

    depth = W_DEPTH

    load_tok.start()
    for copy in cu_loads(0):
        copy.start()
    w_load(0).start()
    barrier = pltpu.get_barrier_semaphore()
    even = lax.rem(z, 2) == 0
    NEAR, ACROSS, MATE = range(3)

    def tell(sem, chip):
        for cr in range(CORES):
            pl.semaphore_signal(sem, inc=1, device_id=(chip * CORES + cr, t), device_id_type=MESH)

    @pl.when(even)
    def _():
        tell(barrier, near)

    @pl.when(half == 0)
    def _():
        tell(barrier, across)

        @inner_only
        def _():
            tell(barrier, far)

    @pl.when(core == 0)
    def _():
        pl.semaphore_signal(barrier, inc=1, device_id=(mate, t), device_id_type=MESH)
    for k in range(1, nt):
        @pl.when(flip(t, k) > t)
        def _():
            pl.semaphore_signal(barrier, inc=1, device_id=(d, flip(t, k)), device_id_type=MESH)

    @phase
    def meet():
        earlier = CORES * (z - half * lax.rem(z, 2)) + t + core

        @pl.when(earlier > 0)
        def _():
            pl.semaphore_wait(barrier, earlier)

    @pl.when(jnp.logical_not(even))
    def _():
        tell(go.at[NEAR], near)

    @pl.when(half == 1)
    def _():
        @inner_only
        def _():
            tell(go.at[ACROSS], across)
            tell(go.at[ACROSS], far)

    @pl.when(core == 1)
    def _():
        pl.semaphore_signal(go.at[MATE], inc=1, device_id=(mate, t), device_id_type=MESH)
    for k in range(1, nt):
        @pl.when(flip(t, k) < t)
        def _():
            pl.semaphore_signal(go.at[MATE + k], inc=1, device_id=(d, flip(t, k)), device_id_type=MESH)

    @phase
    def tok_load():
        load_tok.wait()

    for c in range(1, depth):
        w_load(c).start()

    for k in range(1, nt):
        pl.when(flip(t, k) < t)(tok_copy(k).start)

    def send_down(c):
        @pl.when(half == 1)
        def _():
            to_across(c, A).start()

        @pl.when(jnp.logical_not(even))
        def _():
            send_near(c, A)

    def send_up(c):
        @pl.when(half == 0)
        def _():
            to_across(c, A).start()

        @pl.when(even)
        def _():
            send_near(c, A)

    def own_chunk(c):
        w_load(c).wait()

        @pl.when(c + depth < nc)
        def _():
            w_load(c + depth).start()

        @pl.when(c == nc // 2)
        def _():
            for k in range(1, nt):
                for copy in cu_loads(k):
                    copy.start()
        grads(c, A)

    @phase
    def own_loads():
        cu_wait(True)

    alone = min(ALONE, ng)

    @phase
    def own_first():
        @pl.loop(0, alone)
        def _(c):
            own_chunk(c)

            @pl.when(c > 0)
            def _():
                send_down(c - 1)

    @phase
    def go_wait():
        for k in range(1, nt):
            @pl.when(flip(t, k) > t)
            def _():
                pl.semaphore_wait(go.at[MATE + k], 1)
                tok_copy(k).start()
        send_down(alone - 1)

        @pl.when(even)
        def _():
            pl.semaphore_wait(go.at[NEAR], CORES)

        @pl.when(half == 0)
        def _():
            pl.semaphore_wait(go.at[ACROSS], CORES)

        @pl.when(core == 0)
        def _():
            pl.semaphore_wait(go.at[MATE], 1)

        @pl.loop(0, alone)
        def _(c):
            send_up(c)

    @phase
    def own_grads():
        @pl.loop(alone, nc)
        def _(c):
            own_chunk(c)

            @pl.when(jnp.logical_and(c > alone, c <= ng))
            def _():
                send_first(c - 1)

    load_x.start()
    inner_only(load_xp.start)
    load_m1.start()
    load_m2.start()
    for cr in range(CORES):
        xp_across(cr).start()
    for cr in range(CORES):
        x_across(cr).start()
        x_near(cr).start()
    x_mate.start()
    inner_only(xp_mate.start)

    @pl.loop(ng, nc)
    def _(c):
        send_first(c)

    @phase
    def inner_forwards():
        @inner_only
        def _():
            @pl.loop(0, EARLY_LAG)
            def _(c):
                rest_in(c, A)
                forward(c, A)

            @phase
            def early_wait():
                cu_wait(False)
                tok_early.wait_recv()

            @pl.loop(0, ns)
            def _(c):
                grads(c, B_EARLY)
                rest_in(EARLY_LAG + c, A)
                forward(EARLY_LAG + c, A)
                to_near(c, B_EARLY).start()

            @pl.loop(EARLY_LAG + ns, ng)
            def _(c):
                rest_in(c, A)
                forward(c, A)

        @outer_only
        def _():
            cu_wait(False)
            tok_early.wait_recv()

    @phase
    def tok_wait():
        tok_late.wait_recv()

    @phase
    def other_grads():
        @inner_only
        def _():
            @pl.loop(0, ns)
            def _(c):
                grads(c, B_LATE)

                @pl.when(c > 0)
                def _():
                    send_rest(c - 1, B_LATE)
            grads(ns, B)
            send_rest(ns - 1, B_LATE)

        @outer_only
        def _():
            @pl.loop(0, ns + 1)
            def _(c):
                grads(c, B)

                @pl.when(c > 0)
                def _():
                    send_rest(c - 1)

        @pl.loop(ns + 1, nc)
        def _(c):
            grads(c, B)
            send_rest(c - 1)

    @phase
    def x_exchange():
        term_part(0)
        send_rest(nc - 1)
        load_x.wait()

        @inner_only
        def _():
            xp_beyond.wait_recv()
            x_forward.start()
            load_xp.wait()
            xp_mate.wait_recv()
            x_all.wait_recv()
            for k in range(1, nt):
                x2_copy(k).start()
            for k in range(1, nt):
                xp2_copy(k).start()

    @phase
    def terms():
        @pl.loop(1, nc)
        def _(n):
            term_part(n)

    @phase
    def outer_x():
        @outer_only
        def _():
            x_all.wait_recv()
            for k in range(1, nt):
                x2_copy(k).start()
            for k in range(1, nt):
                term_copy(k).start()

    def takes(c):
        @phase
        def others_in():
            near_in(c)
            mate_copy(c, near).start()

            @outer_only
            def _():
                rest_in(c, A)
            rest_in(c, B)

            @inner_only
            def _():
                forward(c, B)
            mate_copy(c, across).start()
            mate_copy(c, far).start()

    @pl.loop(0, lead)
    def _(c):
        takes(c)

    @inner_only
    def _():
        for k in range(1, nt):
            term_copy(k).start()

    @phase
    def x_wait():
        x2_all.wait_recv()

    load_m1.wait()
    load_m2.wait()

    @phase
    def transposes():
        for i in range(ndp):
            xt[:, i * g:(i + 1) * g] = xg[:, i].reshape(g, rw).T

    @pl.loop(lead, ng)
    def _(c):
        takes(c)

        @phase
        def updates():
            update(c - lead)

    def input_grads():
        with jax.named_scope("input_grads"):
            total = term[0:m, :].astype(F32)
            term_in.wait_recv()
            for k in range(1, nt):
                total += termr[k].astype(F32)
            in_grad[...] = total.astype(BF16)

    @inner_only
    def _():
        @phase
        def xp_wait():
            xp2_all.wait_recv()
            for i in range(others):
                xtp[:, i * g:(i + 1) * g] = xp[:, i].reshape(g, rw).T

        for j in range(nr):
            @phase
            def last_in():
                rest_in(ng + j, A)
                rest_in(ng + j, B)
                mate_copy(ng + j, across).start()
                mate_copy(ng + j, far).start()

            @phase
            def updates():
                update(ng - lead + j)

            @phase
            def reduces():
                reduce(ng + j, j)

            @phase
            def near_last():
                near_in(ng + j)
                mate_last(j).start()

        @pl.loop(ng - lead + nr, ng)
        def _(c):
            update(c)

        @pl.loop(ng, nc)
        def _(c):
            update(c, True)
        input_grads()

    @outer_only
    def _():
        @pl.loop(ng - lead, ng)
        def _(c):
            @phase
            def updates():
                update(c)
        input_grads()
        for j in range(nr):
            @phase
            def finishes():
                finish(ng + j, j)

    def sent(sem, chunks, replicas):
        b = gall.at[0:chunks, 0:replicas * g]
        rdma(b, b, sem, sem, mate, t).wait_send()

    @phase
    def drain():
        tok_all.wait_send()
        x2_all.wait_send()
        term_out.wait_send()
        x_all.wait_send()
        sent(zs.at[1], nc, 1)
        sent(ms.at[0], nc, 1)

        @outer_only
        def _():
            sent(zs.at[0], nc, 1)
            sent(ms.at[1], ng, 3)

        @inner_only
        def _():
            sent(zs.at[0], ng, 1)
            sent(ms.at[1], nc, 3)
            sent(fs.at[0], ng, 2)
            xp_mate.wait_send()
            x_forward.wait_send()
            xp2_all.wait_send()
            rdma(part_s, part_s, rs.at[0], rs.at[0], mate, t).wait_send()


def fused(ndp, nt, tokens, gate_weight, up_act, cotangent, moment1, moment2):
    m, dw = tokens.shape
    g, hid = up_act.shape
    rw = moment1.shape[0]
    nc = hid // WIDE
    nr = SUMMED * nc // 8
    any_spec, vmem = pl.BlockSpec(memory_space=pltpu.HBM), pl.BlockSpec(memory_space=pltpu.VMEM)
    dma = pltpu.SemaphoreType.DMA
    results = (((m, dw), BF16), ((g, hid), BF16), ((rw, hid), BF16), ((rw, hid), BF16), ((rw, hid), F32))
    held = pl.pallas_call(
        functools.partial(kernel, ndp, nt),
        out_shape=tuple(pltpu.VMEM(shape, dtype) for shape, dtype in results),
        in_specs=[any_spec] * 6,
        out_specs=(vmem,) * 5,
        scratch_shapes=[
            pltpu.VMEM((g, dw), BF16),
            pltpu.VMEM((nt, ndp, m, rw), BF16),
            pltpu.VMEM((nt, ndp - CORES, m, rw), BF16),
            pltpu.VMEM((rw, ndp * g), BF16),
            pltpu.VMEM((rw, (ndp - CORES) * g), BF16),
            pltpu.VMEM((nc, dw, WIDE), BF16),
            pltpu.VMEM((g, hid), BF16),
            pltpu.VMEM((g, hid), BF16),
            pltpu.VMEM((rw, hid), BF16),
            pltpu.VMEM((rw, hid), BF16),
            pltpu.VMEM((nc, ndp * g, WIDE), BF16),
            pltpu.VMEM((g, dw), BF16),
            pltpu.VMEM((nt, m, dw), BF16),
            pltpu.VMEM((nr, rw, WIDE), BF16),
            pltpu.VMEM((nr, rw, WIDE), BF16),
            dma((5,)), dma((W_DEPTH,)), dma((3,)), dma((3,)), dma((6,)), dma((4,)),
            dma((2,)), dma((1,)), dma((2,)), dma((nc,)), dma((2, nc)),
            dma((nc + nr,)), dma((1,)), dma((nr, 2)), dma((2,)), pltpu.SemaphoreType.REGULAR((2 + nt,)),
        ],
        compiler_params=pltpu.CompilerParams(
            collective_id=0, has_side_effects=True, vmem_limit_bytes=VMEM_BUDGET),
    )(*(pltpu.with_memory_space_constraint(x, pltpu.HBM)
        for x in (tokens, gate_weight, up_act, cotangent, moment1, moment2)))
    return pl.pallas_call(
        write_out,
        out_shape=tuple(pltpu.HBM(shape, dtype) for shape, dtype in results),
        in_specs=[vmem] * 5,
        out_specs=(any_spec,) * 5,
        scratch_shapes=[dma((5,))],
        compiler_params=pltpu.CompilerParams(vmem_limit_bytes=2**20),
    )(*(pltpu.with_memory_space_constraint(x, pltpu.VMEM) for x in held))


def write_out(*refs):
    sems = refs[-1]
    copies = [pltpu.make_async_copy(refs[i], refs[5 + i], sems.at[i]) for i in range(5)]
    for copy in reversed(copies):
        copy.start()
    for copy in copies:
        copy.wait()


def plain(ndp, nt, tokens, gate_weight, up_act, cotangent, moment1, moment2):
    gathered = lax.all_gather(tokens, "tensor", axis=0, tiled=True)
    gate_pre = jnp.dot(gathered, gate_weight, preferred_element_type=F32)
    up_grad, gate_grad = activation_grads(gate_pre, cotangent, up_act)
    term = lax.dot_general(
        gate_grad, gate_weight, (((1,), (1,)), ((), ())), preferred_element_type=F32).astype(BF16)
    in_grad = lax.psum_scatter(term, "tensor", scatter_dimension=0, tiled=True)
    partial_value = lax.dot_general(
        gathered, gate_grad, (((0,), (0,)), ((), ())), preferred_element_type=F32).astype(BF16)
    shard = lax.psum_scatter(partial_value.astype(F32), "dp", scatter_dimension=0, tiled=True)
    first, second, update = adam(shard * (1.0 / math.sqrt(ndp * gathered.shape[0])), moment1, moment2)
    return in_grad, up_grad, first.astype(BF16), second.astype(BF16), update


def local(ndp, nt, *args):
    (m, dw), (g, hid), rw = args[0].shape, args[2].shape, args[4].shape[0]
    need = (2 * dw * hid + 2 * ndp * g * (hid + 2 * rw) + 12 * g * hid + 16 * rw * hid + 16 * g * dw)
    fits = (need <= VMEM_BUDGET and hid >= 8 * WIDE and ndp == CORES * CHIPS and nt > 1 and nt & (nt - 1) == 0
            and hid % WIDE == 0 and g % 128 == 0 and rw % 128 == 0 and m % 16 == 0
            and dw % (128 * (hid // WIDE)) == 0)
    return (fused if fits else plain)(ndp, nt, *args)


def solution(mesh):
    both = P("dp", "tensor")
    rows = P(("dp", "tensor"), None)
    return jax.shard_map(
        functools.partial(local, mesh.shape["dp"], mesh.shape["tensor"]),
        mesh=mesh,
        in_specs=(rows, P(None, "tensor"), both, both, both, both),
        out_specs=(rows, both, both, both, both),
        check_vma=False,
    )
```
